32 devices in a mesh: dp: 2 (over x), tp: 4 (over z), ep: 4 (over y, core).
Axes of the slice: x: 2, y: 2, z: 4, core: 2. Of those that a mesh axis runs over, the one named last changes fastest.
Arguments:
- hidden_in: bfloat16 [8192, 2048], P(('dp', 'ep')), parts along dimension 0
- topk_idx: int32 [8192, 4], P(('dp', 'ep')), parts along dimension 0
- norm_gain: bfloat16 [2048], replicated
- router_w: bfloat16 [2048, 60], replicated
- shared_sig_w: bfloat16 [2048, 1], replicated
- exp_gate: bfloat16 [60, 2048, 1408], P('ep', None, 'tp')
- exp_up: bfloat16 [60, 2048, 1408], P('ep', None, 'tp')
- exp_down: bfloat16 [60, 1408, 2048], P('ep', 'tp')
- sh_gate: bfloat16 [2048, 5632], P(None, ('tp', 'ep'))
- sh_up: bfloat16 [2048, 5632], P(None, ('tp', 'ep'))
- sh_down: bfloat16 [5632, 2048], P(('tp', 'ep'))
Outputs:
- output: bfloat16 [8192, 2048], P(('dp', 'ep')), parts along dimension 0
There are 2 independent parts. The reference program is written for one: setup_inputs(seed, part) draws one part's arguments, and reference() takes and returns one part's arrays. A program takes and returns all parts, laid end to end along the dimension named above; an argument that names none is the same for every part.
All inputs are finite; a program needn't handle non-finite values.
Results may differ from the reference program's by a relative error of at most 0.0110312.
Values are sent between devices in bfloat16 or wider.
A program may use at most 1 GiB of HBM per device.

```python
import jax
import jax.numpy as jnp
from jax import lax

HIDDEN = 2048
EXPERTS = 60
TOP_K = 4
EXPERT_WIDTH = 1408
SHARED_WIDTH = 5632
TOKENS = 4096
ROW_BLOCK = 128
RMS_EPS = 1e-6


def setup_inputs(seed: int = 0, part: int = 0) -> dict:
    weight_keys = jax.random.split(jax.random.key(seed), 9)
    part_keys = jax.random.split(jax.random.fold_in(jax.random.key(seed + 1), part), 3)
    hidden_in = jax.random.normal(part_keys[0], (TOKENS, HIDDEN), jnp.float32)
    hot_bias = jax.random.randint(part_keys[1], (EXPERTS,), 0, 3) * 400
    noise_score = jax.random.randint(part_keys[2], (TOKENS, EXPERTS), 0, 1000)
    ranked = (noise_score + hot_bias[None, :]) * EXPERTS + jnp.arange(EXPERTS)[None, :]
    topk_idx = lax.top_k(ranked, TOP_K)[1].astype(jnp.int32)
    in_scale = HIDDEN ** -0.5
    down_scale = 0.7 * EXPERTS * TOP_K ** -0.5 * EXPERT_WIDTH ** -0.5
    shared_scale = 2.0 * SHARED_WIDTH ** -0.5
    norm_gain = jax.random.uniform(weight_keys[0], (HIDDEN,), jnp.float32, 0.5, 1.5)
    router_w = jax.random.normal(weight_keys[1], (HIDDEN, EXPERTS), jnp.float32) * in_scale
    shared_sig_w = jax.random.normal(weight_keys[2], (HIDDEN, 1), jnp.float32) * in_scale
    exp_gate = jax.random.normal(weight_keys[3], (EXPERTS, HIDDEN, EXPERT_WIDTH), jnp.float32) * in_scale
    exp_up = jax.random.normal(weight_keys[4], (EXPERTS, HIDDEN, EXPERT_WIDTH), jnp.float32) * in_scale
    exp_down = jax.random.normal(weight_keys[5], (EXPERTS, EXPERT_WIDTH, HIDDEN), jnp.float32) * down_scale
    sh_gate = jax.random.normal(weight_keys[6], (HIDDEN, SHARED_WIDTH), jnp.float32) * in_scale
    sh_up = jax.random.normal(weight_keys[7], (HIDDEN, SHARED_WIDTH), jnp.float32) * in_scale
    sh_down = jax.random.normal(weight_keys[8], (SHARED_WIDTH, HIDDEN), jnp.float32) * shared_scale
    return {
        'hidden_in': hidden_in.astype(jnp.bfloat16),
        'topk_idx': topk_idx,
        'norm_gain': norm_gain.astype(jnp.bfloat16),
        'router_w': router_w.astype(jnp.bfloat16),
        'shared_sig_w': shared_sig_w.astype(jnp.bfloat16),
        'exp_gate': exp_gate.astype(jnp.bfloat16),
        'exp_up': exp_up.astype(jnp.bfloat16),
        'exp_down': exp_down.astype(jnp.bfloat16),
        'sh_gate': sh_gate.astype(jnp.bfloat16),
        'sh_up': sh_up.astype(jnp.bfloat16),
        'sh_down': sh_down.astype(jnp.bfloat16),
    }


def rms_norm(rows, gain):
    rows_f32 = rows.astype(jnp.float32)
    inv_rms = lax.rsqrt(jnp.mean(rows_f32 * rows_f32, axis=-1, keepdims=True) + RMS_EPS)
    return (rows_f32 * inv_rms * gain.astype(jnp.float32)).astype(jnp.bfloat16)


def routed_sum(normed, topk_idx, chosen_wt, exp_gate, exp_up, exp_down):
    n_tok, n_top = topk_idx.shape
    n_rows = n_tok * n_top
    block_rows = min(ROW_BLOCK, n_rows)
    flat_exp = topk_idx.reshape(-1)
    order = jnp.argsort(flat_exp, stable=True)
    row_tok = order // n_top
    row_wt = chosen_wt.reshape(-1)[order]
    counts = jax.ops.segment_sum(jnp.ones_like(flat_exp), flat_exp, num_segments=EXPERTS)
    starts = jnp.cumsum(counts) - counts

    def per_expert(running, expert_xs):
        w_gate, w_up, w_down, first, count = expert_xs

        def body(step, acc_in):
            row_start = first + step * block_rows
            begin = jnp.minimum(row_start, n_rows - block_rows)
            positions = begin + jnp.arange(block_rows)
            keep = (positions >= row_start) & (positions < first + count)
            tok_ids = lax.dynamic_slice(row_tok, (begin,), (block_rows,))
            row_wts = jnp.where(keep, lax.dynamic_slice(row_wt, (begin,), (block_rows,)), 0.0)
            rows = normed[tok_ids]
            gate_val = jnp.dot(rows, w_gate, preferred_element_type=jnp.float32)
            up_val = jnp.dot(rows, w_up, preferred_element_type=jnp.float32)
            act_val = (jax.nn.silu(gate_val) * up_val).astype(jnp.bfloat16)
            down_val = jnp.dot(act_val, w_down, preferred_element_type=jnp.float32)
            return acc_in.at[tok_ids].add(down_val * row_wts[:, None])

        n_steps = (count + block_rows - 1) // block_rows
        return lax.fori_loop(0, n_steps, body, running), None

    zeros_init = jnp.zeros((n_tok, HIDDEN), jnp.float32)
    total, _ = lax.scan(per_expert, zeros_init, (exp_gate, exp_up, exp_down, starts, counts))
    return total


def reference(hidden_in, topk_idx, norm_gain, router_w, shared_sig_w, exp_gate, exp_up, exp_down, sh_gate, sh_up, sh_down):
    normed = rms_norm(hidden_in, norm_gain)
    router_prob = jax.nn.softmax(jnp.dot(normed, router_w, preferred_element_type=jnp.float32), axis=-1)
    chosen_wt = jnp.take_along_axis(router_prob, topk_idx, axis=1)
    routed = routed_sum(normed, topk_idx, chosen_wt, exp_gate, exp_up, exp_down)
    sig_gate = jax.nn.sigmoid(jnp.dot(normed, shared_sig_w, preferred_element_type=jnp.float32))
    sh_act = (jax.nn.silu(jnp.dot(normed, sh_gate, preferred_element_type=jnp.float32)) * jnp.dot(normed, sh_up, preferred_element_type=jnp.float32)).astype(jnp.bfloat16)
    shared = sig_gate * jnp.dot(sh_act, sh_down, preferred_element_type=jnp.float32)
    return (hidden_in.astype(jnp.float32) + routed + shared).astype(jnp.bfloat16)
```

```python
import functools

import jax
import jax.numpy as jnp
from jax import lax
from jax.experimental import pallas as pl
from jax.experimental.pallas import tpu as pltpu
from jax.sharding import PartitionSpec as P

RMS_EPS = 1e-6
LANES = 128
TILE = 256
PITCH = TILE + 1
GROUP = 8
MESH = pl.DeviceIdType.MESH
SPREAD_CHUNKS = 8
COMBINE_CHUNKS = 32
COMBINE_LAG = 2


def rms_norm(rows, gain):
    rows_f32 = rows.astype(jnp.float32)
    inv_rms = lax.rsqrt(jnp.mean(rows_f32 * rows_f32, axis=-1, keepdims=True) + RMS_EPS)
    return (rows_f32 * inv_rms * gain.astype(jnp.float32)).astype(jnp.bfloat16)


def dot_t(a, b):
    return lax.dot_general(a, b, (((1,), (1,)), ((), ())), preferred_element_type=jnp.float32)


def moe_kernel(start_ref, count_ref, tok_ref, wt_ref, h_hbm, eg, eu, ed, sg, su, sd, out_hbm,
               hv, acc, wg, wu, wd, x4, xb, act, y4, h_sem, w_sem, o_sem):
    n_tok, chunks, _ = hv.shape
    n_exp = eg.shape[0]

    def weight_copies(e, slot, shared):
        srcs = (sg, su, sd) if shared else (eg.at[e - 1], eu.at[e - 1], ed.at[e - 1])
        return [pltpu.make_async_copy(s, d.at[slot], w_sem.at[slot, i])
                for i, (s, d) in enumerate(zip(srcs, (wg, wu, wd)))]

    h_copy = pltpu.make_async_copy(h_hbm, hv, h_sem)
    h_copy.start()
    for c in weight_copies(0, 0, True):
        c.start()

    zero = jnp.zeros((16, chunks, LANES), jnp.float32)

    def clear(i, _):
        acc[pl.ds(i * 16, 16)] = zero
        return 0
    lax.fori_loop(0, n_tok // 16, clear, 0)
    h_copy.wait()

    def tile_body(base, n, slot):
        def gather(g, _):
            for u in range(GROUP):
                i = g * GROUP + u
                tok = tok_ref[base + i]
                x4[pl.ds(i, chunks, stride=PITCH), :] = hv[tok].astype(jnp.float32)
            return 0
        lax.fori_loop(0, TILE // GROUP, gather, 0)
        for k in range(chunks):
            xb[:, k * LANES:(k + 1) * LANES] = x4[k * PITCH:k * PITCH + TILE, :].astype(jnp.bfloat16)
        gate = dot_t(xb[...], wg[slot])
        up = dot_t(xb[...], wu[slot])
        act[...] = (jax.nn.silu(gate) * up).astype(jnp.bfloat16)
        for k in range(0, chunks, 2):
            d = jnp.dot(act[...], wd[slot, :, k * LANES:(k + 2) * LANES], preferred_element_type=jnp.float32)
            y4[k * PITCH:k * PITCH + TILE, :] = d[:, :LANES]
            y4[(k + 1) * PITCH:(k + 1) * PITCH + TILE, :] = d[:, LANES:]

        def scatter(g, _):
            sums = []
            for u in range(GROUP):
                i = g * GROUP + u
                tok = jnp.where(i < n, tok_ref[base + i], n_tok + u)
                sums.append((tok, acc[tok] + y4[pl.ds(i, chunks, stride=PITCH), :] * wt_ref[base + i]))
            for tok, v in sums:
                acc[tok] = v
            return 0
        lax.fori_loop(0, (n + GROUP - 1) // GROUP, scatter, 0)

    def expert(e, _):
        slot = lax.rem(e, 2)
        count = count_ref[e]

        @pl.when(count > 0)
        def _():
            for c in weight_copies(0, slot, True):
                c.wait()

        nxt = jnp.minimum(e + 1, n_exp)

        @pl.when((e < n_exp) & (count_ref[nxt] > 0))
        def _():
            for c in weight_copies(nxt, 1 - slot, False):
                c.start()

        def tile(t, _):
            tile_body(start_ref[e] + t * TILE, jnp.minimum(count - t * TILE, TILE), slot)
            return 0
        lax.fori_loop(0, (count + TILE - 1) // TILE, tile, 0)
        return 0

    lax.fori_loop(0, n_exp + 1, expert, 0)

    blk = 256

    def flush(i, _):
        def conv(j, _):
            r = i * blk + j * 8
            hv[pl.ds(r, 8)] = acc[pl.ds(r, 8)].astype(jnp.bfloat16)
            return 0
        lax.fori_loop(0, blk // 8, conv, 0)
        pltpu.make_async_copy(hv.at[pl.ds(i * blk, blk)], out_hbm.at[pl.ds(i * blk, blk)], o_sem).start()
        return 0
    lax.fori_loop(0, n_tok // blk, flush, 0)
    pltpu.make_async_copy(hv, out_hbm, o_sem).wait()


def moe(start, count, tok, wt, h3, eg, eu, ed, sg, su, sd):
    n_tok, chunks, _ = h3.shape
    hidden = chunks * LANES
    width = ed.shape[1]
    n_exp = eg.shape[0]
    smem = pl.BlockSpec(memory_space=pltpu.SMEM)
    hbm = pl.BlockSpec(memory_space=pl.ANY)
    flops = 2 * 3 * hidden * width * 2 * n_tok
    return pl.pallas_call(
        moe_kernel,
        out_shape=jax.ShapeDtypeStruct((n_tok, chunks, LANES), jnp.bfloat16),
        in_specs=[smem] * 4 + [hbm] * 7,
        out_specs=hbm,
        scratch_shapes=[
            pltpu.VMEM((n_tok, chunks, LANES), jnp.bfloat16),
            pltpu.VMEM((n_tok + GROUP, chunks, LANES), jnp.float32),
            pltpu.VMEM((2, width, hidden), jnp.bfloat16),
            pltpu.VMEM((2, width, hidden), jnp.bfloat16),
            pltpu.VMEM((2, width, hidden), jnp.bfloat16),
            pltpu.VMEM((chunks * PITCH + 8, LANES), jnp.float32),
            pltpu.VMEM((TILE, hidden), jnp.bfloat16),
            pltpu.VMEM((TILE, width), jnp.bfloat16),
            pltpu.VMEM((chunks * PITCH + 8, LANES), jnp.float32),
            pltpu.SemaphoreType.DMA,
            pltpu.SemaphoreType.DMA((2, 3)),
            pltpu.SemaphoreType.DMA,
        ],
        compiler_params=pltpu.CompilerParams(vmem_limit_bytes=67043328),
        cost_estimate=pl.CostEstimate(flops=flops, bytes_accessed=110_000_000, transcendentals=0),
        name="moe",
    )(start, count, tok, wt, h3, eg, eu, ed, sg, su, sd)


def spread_kernel(n_chunk, h_ref, out_ref, own_sem, pair_send, pair_recv, y_send, y_recv, z_send, z_recv, fwd_send, fwd_recv):
    z, e = lax.axis_index("tp"), lax.axis_index("ep")
    rows = h_ref.shape[0]
    size = rows // (2 * n_chunk)
    core = e % 2
    pair = e + 1 - 2 * core
    far = (e + 2) % 4
    half = z % 2
    zpair = z + 1 - 2 * half

    barrier = pltpu.get_barrier_semaphore()
    for dev in ({"ep": pair}, {"ep": far}, {"tp": zpair}):
        pl.semaphore_signal(barrier, inc=1, device_id=dev, device_id_type=MESH)
    pl.semaphore_wait(barrier, 3)

    def y_copy(j):
        lo = half * (rows // 2) + j * size
        return pltpu.make_async_remote_copy(
            h_ref.at[pl.ds(lo, size)], out_ref.at[pl.ds(e * rows + lo, size)],
            y_send.at[j], y_recv.at[j], device_id={"ep": far}, device_id_type=MESH)

    def far_rows(j, h):
        return out_ref.at[pl.ds(far * rows + h * (rows // 2) + j * size, size)]

    def z_copy(j):
        return pltpu.make_async_remote_copy(
            far_rows(j, half), far_rows(j, half), z_send.at[j], z_recv.at[j], device_id={"tp": zpair}, device_id_type=MESH)

    def fwd_copy(j, side):
        h = half if side == 0 else 1 - half
        return pltpu.make_async_remote_copy(
            far_rows(j, h), far_rows(j, h), fwd_send.at[side, j], fwd_recv.at[side, j], device_id={"ep": pair}, device_id_type=MESH)

    own = pltpu.make_async_copy(h_ref, out_ref.at[pl.ds(e * rows, rows)], own_sem)
    to_pair = pltpu.make_async_remote_copy(
        h_ref, out_ref.at[pl.ds(e * rows, rows)], pair_send, pair_recv, device_id={"ep": pair}, device_id_type=MESH)

    def send(j, _):
        y_copy(j).start()
        return 0
    lax.fori_loop(0, n_chunk, send, 0)
    to_pair.start()
    own.start()

    def relay(i, _):
        @pl.when(i < n_chunk)
        def _():
            y_copy(i).wait_recv()
            z_copy(i).start()
            fwd_copy(i, 0).start()

        @pl.when(i >= 2)
        def _():
            z_copy(i - 2).wait_recv()
            fwd_copy(i - 2, 1).start()
        return 0
    lax.fori_loop(0, n_chunk + 2, relay, 0)

    def drain(j, _):
        fwd_copy(j, 0).wait()
        fwd_copy(j, 1).wait()
        y_copy(j).wait_send()
        z_copy(j).wait_send()
        return 0
    lax.fori_loop(0, n_chunk, drain, 0)
    to_pair.wait()
    own.wait()


def spread(h3, ranks, n_chunk):
    rows = h3.shape[0]
    dma = pltpu.SemaphoreType.DMA
    return pl.pallas_call(
        functools.partial(spread_kernel, n_chunk),
        out_shape=jax.ShapeDtypeStruct((ranks * rows,) + h3.shape[1:], h3.dtype),
        in_specs=[pl.BlockSpec(memory_space=pltpu.VMEM)],
        out_specs=pl.BlockSpec(memory_space=pl.ANY),
        scratch_shapes=[dma, dma, dma, dma((n_chunk,)), dma((n_chunk,)), dma((n_chunk,)), dma((n_chunk,)),
                        dma((2, n_chunk)), dma((2, n_chunk))],
        compiler_params=pltpu.CompilerParams(collective_id=0, has_side_effects=True, vmem_limit_bytes=20 << 20),
        name="spread",
    )(h3)


def combine_kernel(n_chunk, lag, part, hid_hbm, out_ref, mine, near, far_in, zin, hid, t4, m_sem, h_sem,
                   d_send, d_recv, y_send, y_recv, z_send, z_recv, t_send):
    z, e = lax.axis_index("tp"), lax.axis_index("ep")
    rows = out_ref.shape[0]
    chunks = part.shape[1]
    size = rows // n_chunk
    core = e % 2
    pair = e + 1 - 2 * core
    far = (e + 2) % 4
    far_pair = (pair + 2) % 4
    n_z = 4
    zn = z + 1 - 2 * (z % 2)

    barrier = pltpu.get_barrier_semaphore()
    for dev in ({"ep": pair}, {"ep": far}):
        pl.semaphore_signal(barrier, inc=1, device_id=dev, device_id_type=MESH)

    @pl.when(z > 0)
    def _():
        pl.semaphore_signal(barrier, inc=1, device_id={"tp": z - 1}, device_id_type=MESH)

    @pl.when(z < n_z - 1)
    def _():
        pl.semaphore_signal(barrier, inc=1, device_id={"tp": z + 1}, device_id_type=MESH)
    at_end = (z == 0) | (z == n_z - 1)

    @pl.when(at_end)
    def _():
        pl.semaphore_wait(barrier, 3)

    @pl.when(jnp.logical_not(at_end))
    def _():
        pl.semaphore_wait(barrier, 4)

    def at(j):
        return pl.ds(j * size, size)

    def d_copy(j, side):
        owner = far_pair if side == 0 else pair
        return pltpu.make_async_remote_copy(
            part.at[pl.ds(owner * rows + j * size, size)], near.at[side, at(j)],
            d_send.at[side, j], d_recv.at[side, j], device_id={"ep": pair}, device_id_type=MESH)

    def m_copy(j, side):
        owner = far if side == 0 else e
        return pltpu.make_async_copy(part.at[pl.ds(owner * rows + j * size, size)], mine.at[side, at(j)], m_sem.at[side, j])

    def y_copy(j):
        return pltpu.make_async_remote_copy(
            mine.at[0, at(j)], far_in.at[at(j)], y_send.at[j], y_recv.at[j], device_id={"ep": far}, device_id_type=MESH)

    def z_copy(j, slot, to):
        return pltpu.make_async_remote_copy(
            mine.at[1, at(j)], zin.at[slot, at(j)], z_send.at[j], z_recv.at[slot, j], device_id={"tp": to}, device_id_type=MESH)

    def t_copy(j, side, to, src):
        return pltpu.make_async_remote_copy(
            src, zin.at[1, at(j)], t_send.at[side, j], z_recv.at[1, j], device_id={"tp": to}, device_id_type=MESH)

    hid_copy = pltpu.make_async_copy(hid_hbm, hid, h_sem)

    def first(j, _):
        for side in range(2):
            d_copy(j, side).start()
            m_copy(j, side).start()
        return 0
    lax.fori_loop(0, n_chunk, first, 0)
    hid_copy.start()
    hid_copy.wait()

    def f32(ref):
        return ref[...].astype(jnp.float32)

    def finish(j, src):
        def put(g, _):
            for u in range(8):
                i = g * 8 + u
                t4[pl.ds(i, chunks, stride=size + 1), :] = src[i].astype(jnp.float32)
            return 0
        lax.fori_loop(0, size // 8, put, 0)
        for k in range(chunks):
            cols = slice(k * LANES, (k + 1) * LANES)
            tot = t4[k * (size + 1):k * (size + 1) + size, :]
            out_ref[at(j), cols] = (hid[at(j), cols].astype(jnp.float32) + tot).astype(jnp.bfloat16)

    def step(i, _):
        @pl.when(i < n_chunk)
        def _():
            for side in range(2):
                d_copy(i, side).wait_recv()
                m_copy(i, side).wait()
            mine[0, at(i)] = (f32(mine.at[0, at(i)]) + f32(near.at[0, at(i)])).astype(jnp.bfloat16)
            y_copy(i).start()

        def stage(shift):
            j = i - shift * lag
            odd = j % 2
            spot = z + odd * (n_z - 1 - 2 * z)
            ahead = 1 - 2 * odd
            return j, spot, ahead, (j >= 0) & (j < n_chunk)

        j, spot, ahead, live = stage(1)

        @pl.when(live)
        def _():
            y_copy(j).wait_recv()
            mine[1, at(j)] = (f32(mine.at[1, at(j)]) + f32(near.at[1, at(j)]) + f32(far_in.at[at(j)])).astype(jnp.bfloat16)

            @pl.when(spot == 0)
            def _():
                z_copy(j, 0, z + ahead).start()

            @pl.when(spot == 3)
            def _():
                z_copy(j, 0, z - ahead).start()

        j2, spot2, ahead2, live2 = stage(2)

        @pl.when(live2 & (spot2 == 2))
        def _():
            z_copy(j2, 0, zn).wait_recv()
            mine[1, at(j2)] = (f32(mine.at[1, at(j2)]) + f32(zin.at[0, at(j2)])).astype(jnp.bfloat16)
            z_copy(j2, 1, z - ahead2).start()

        j3, spot3, ahead3, live3 = stage(3)

        @pl.when(live3 & (spot3 == 1))
        def _():
            z_copy(j3, 0, zn).wait_recv()
            z_copy(j3, 1, zn).wait_recv()
            mine[1, at(j3)] = (f32(mine.at[1, at(j3)]) + f32(zin.at[0, at(j3)]) + f32(zin.at[1, at(j3)])).astype(jnp.bfloat16)
            t_copy(j3, 0, z - ahead3, mine.at[1, at(j3)]).start()
            t_copy(j3, 1, z + ahead3, mine.at[1, at(j3)]).start()
            finish(j3, mine.at[1, at(j3)])

        j4, spot4, ahead4, live4 = stage(4)

        @pl.when(live4 & (spot4 == 2))
        def _():
            z_copy(j4, 1, zn).wait_recv()
            t_copy(j4, 0, z + ahead4, zin.at[1, at(j4)]).start()
            finish(j4, zin.at[1, at(j4)])

        j5, spot5, ahead5, live5 = stage(5)

        @pl.when(live5 & ((spot5 == 0) | (spot5 == 3)))
        def _():
            z_copy(j5, 1, zn).wait_recv()
            finish(j5, zin.at[1, at(j5)])
        return 0
    lax.fori_loop(0, n_chunk + 5 * lag, step, 0)

    def drain(j, _):
        odd = j % 2
        spot = z + odd * (n_z - 1 - 2 * z)
        d_copy(j, 0).wait_send()
        d_copy(j, 1).wait_send()
        y_copy(j).wait_send()

        @pl.when(spot != 1)
        def _():
            z_copy(j, 0, zn).wait_send()

        @pl.when((spot == 1) | (spot == 2))
        def _():
            t_copy(j, 0, zn, mine.at[1, at(j)]).wait_send()

        @pl.when(spot == 1)
        def _():
            t_copy(j, 1, zn, mine.at[1, at(j)]).wait_send()
        return 0
    lax.fori_loop(0, n_chunk, drain, 0)


def combine(part, hidden_in, n_chunk, lag):
    rows, hidden = hidden_in.shape
    block = (rows,) + part.shape[1:]
    dma = pltpu.SemaphoreType.DMA
    size = rows // n_chunk
    hbm = pl.BlockSpec(memory_space=pl.ANY)
    return pl.pallas_call(
        functools.partial(combine_kernel, n_chunk, lag),
        out_shape=jax.ShapeDtypeStruct((rows, hidden), jnp.bfloat16),
        in_specs=[hbm, hbm],
        out_specs=pl.BlockSpec(memory_space=pltpu.VMEM),
        scratch_shapes=[
            pltpu.VMEM((2,) + block, jnp.bfloat16), pltpu.VMEM((2,) + block, jnp.bfloat16), pltpu.VMEM(block, jnp.bfloat16),
            pltpu.VMEM((2,) + block, jnp.bfloat16), pltpu.VMEM((rows, hidden), jnp.bfloat16),
            pltpu.VMEM(((size + 1) * part.shape[1] + 8, LANES), jnp.float32),
            dma((2, n_chunk)), dma, dma((2, n_chunk)), dma((2, n_chunk)), dma((n_chunk,)), dma((n_chunk,)),
            dma((n_chunk,)), dma((2, n_chunk)), dma((2, n_chunk)),
        ],
        compiler_params=pltpu.CompilerParams(collective_id=1, has_side_effects=True, vmem_limit_bytes=60 << 20),
        name="combine",
    )(part, hidden_in)


def routing(meta, n_local, ep_rank):
    n_tok = meta.shape[0]
    k = (meta.shape[1] - 1) // 2
    ids = meta[:, :k].astype(jnp.int32)
    local = ids - ep_rank * n_local
    is_local = (local >= 0) & (local < n_local)
    key = jnp.where(is_local, local, n_local).reshape(-1)
    n = n_tok * k
    packed = key * n + jnp.arange(n, dtype=jnp.int32)
    packed, wts = lax.sort((packed, meta[:, k:2 * k].reshape(-1)), num_keys=1)
    toks = (packed % n) // k
    counts = jnp.sum((key[None, :] == jnp.arange(n_local)[:, None]).astype(jnp.int32), axis=1)
    starts = n_tok + jnp.cumsum(counts) - counts
    start = jnp.concatenate([jnp.zeros((1,), jnp.int32), starts.astype(jnp.int32)])
    count = jnp.concatenate([jnp.full((1,), n_tok, jnp.int32), counts])
    tok_list = jnp.concatenate([jnp.arange(n_tok, dtype=jnp.int32), toks, jnp.zeros((TILE,), jnp.int32)])
    wt_list = jnp.concatenate([meta[:, 2 * k], wts, jnp.zeros((TILE,), jnp.float32)])
    return start, count, tok_list, wt_list


def solution(mesh):
    tok_spec = P(('dp', 'ep'), None)
    in_specs = (tok_spec, tok_spec, P(None), P(None, None), P(None, None),
                P('ep', None, 'tp'), P('ep', None, 'tp'), P('ep', 'tp', None),
                P(None, ('tp', 'ep')), P(None, ('tp', 'ep')), P(('tp', 'ep'), None))

    def local_step(hidden_in, topk_idx, norm_gain, router_w, shared_sig_w, exp_gate, exp_up, exp_down, sh_gate, sh_up, sh_down):
        rows, hidden = hidden_in.shape
        n_exp = router_w.shape[1]
        normed = rms_norm(hidden_in, norm_gain)
        head = jnp.dot(normed, jnp.concatenate([router_w, shared_sig_w], axis=1), preferred_element_type=jnp.float32)
        router_prob = jax.nn.softmax(head[:, :n_exp], axis=-1)
        hit = topk_idx[:, :, None] == jnp.arange(n_exp)[None, None, :]
        chosen_wt = jnp.sum(jnp.where(hit, router_prob[:, None, :], 0.0), axis=-1)
        sig_gate = jax.nn.sigmoid(head[:, n_exp:])
        meta = jnp.concatenate([topk_idx.astype(jnp.float32), chosen_wt, sig_gate], axis=1)
        all_meta = lax.all_gather(meta, 'ep', axis=0, tiled=True)
        h3 = normed.reshape(rows, hidden // LANES, LANES)
        all_h = spread(h3, lax.axis_size('ep'), SPREAD_CHUNKS)
        start, count, tok, wt = routing(all_meta, exp_gate.shape[0], lax.axis_index('ep'))
        part = moe(start, count, tok, wt, all_h, jnp.swapaxes(exp_gate, 1, 2), jnp.swapaxes(exp_up, 1, 2), exp_down,
                   sh_gate.T, sh_up.T, sh_down)
        return combine(part, hidden_in, COMBINE_CHUNKS, COMBINE_LAG)

    return jax.shard_map(local_step, mesh=mesh, in_specs=in_specs, out_specs=tok_spec, check_vma=False)
```

```python
import functools
import math

import jax
import jax.numpy as jnp
from jax import lax
from jax.experimental import pallas as pl
from jax.experimental.pallas import tpu as pltpu
from jax.sharding import PartitionSpec as P

RMS_EPS = 1e-6
LANES = 128
TILE = 256
PITCH = TILE + 1
GROUP = 8
TOK_MASK = 8191
MESH = pl.DeviceIdType.MESH
SPREAD_CHUNKS = 16
COMBINE_CHUNKS = 64
COMBINE_LAG = 3


def dot_t(a, b):
    return lax.dot_general(a, b, (((1,), (1,)), ((), ())), preferred_element_type=jnp.float32)


def routing(idx_ref, first, n_tok, n_local, n_row, pos_v, list_v, in_row, totals):
    n = idx_ref.shape[0]
    i32, bf16, f32 = jnp.int32, jnp.bfloat16, jnp.float32
    sub = lax.broadcasted_iota(i32, (LANES, LANES), 0)
    lane = lax.broadcasted_iota(i32, (LANES, LANES), 1)
    below = jnp.where(sub < lane, 1.0, 0.0).astype(bf16)
    above = jnp.where(lane < sub, 1.0, 0.0).astype(bf16)
    ones = jnp.ones((LANES, LANES), bf16)

    def mask(e):
        return jnp.where(idx_ref[...] == first + e, 1.0, 0.0)

    def count_row(e, _):
        at = pl.ds(pl.multiple_of(e * n, LANES), n)
        hit = mask(e).astype(bf16)
        in_row[at, :] = jnp.dot(hit, below, preferred_element_type=f32)
        totals[at, :] = jnp.dot(hit, ones, preferred_element_type=f32)
        return 0
    lax.fori_loop(0, n_local, count_row, 0)
    pos = jnp.zeros((n, LANES), f32)
    start = jnp.zeros((1, LANES), i32)
    for e in range(n_local):
        total = totals[e * n:(e + 1) * n, :]
        before = jnp.dot(above, total.astype(bf16), preferred_element_type=f32)
        count = (before[n - 1:n] + total[n - 1:n]).astype(i32)
        tiles = (count + TILE - 1) // TILE
        list_v[n_row + e:n_row + e + 1, :] = tiles
        pos += mask(e) * (in_row[e * n:(e + 1) * n, :] + before + (start * TILE).astype(f32) + 1.0)
        start += tiles
    pos_v[...] = pos.astype(i32) - 1

    rows = lax.broadcasted_iota(i32, (n_row, LANES), 0)
    per_k = n_tok // LANES
    base = n_tok // LANES
    lane_val = lax.broadcasted_iota(i32, (LANES, LANES), 1).astype(f32)

    def add(g, acc):
        lhs, rhs = [], []
        for u in range(2):
            r = g * 2 + u
            p = pos_v[pl.ds(r, 1), :]
            code = (r // per_k * ((TOK_MASK + 1) // LANES) + r % per_k - base).astype(f32)
            lhs.append(jnp.where(rows == p // LANES, 1.0, 0.0).astype(bf16))
            hit = sub == jnp.where(p < 0, LANES, p % LANES)
            rhs.append(jnp.concatenate([jnp.where(hit, code, 0.0), jnp.where(hit, lane_val, 0.0)], axis=0).astype(bf16))
        return acc + dot_t(jnp.concatenate(lhs, axis=1), jnp.concatenate(rhs, axis=1))
    acc = lax.fori_loop(0, n // 2, add, jnp.zeros((n_row, 2 * LANES), f32))
    list_v[0:n_row, :] = (acc[:, :LANES] * LANES + acc[:, LANES:]).astype(i32) + n_tok


def moe_kernel(idx_ref, wt_ref, h_hbm, sum_hbm, eg, eu, ed, out_hbm,
               hv, acc, wg, wu, wd, x4, xb, act, y4, pos_v, list_v, list_ref, tile_exp, h_sem, s_sem, w_sem, o_sem, l_sem):
    n_tok, chunks, _ = h_hbm.shape
    n_local = eg.shape[0]
    n_row = list_v.shape[0] - 16
    span = TILE // LANES
    last = n_row // span - 1

    def weight_copies(e, slot):
        return [pltpu.make_async_copy(s.at[e], d.at[slot], w_sem.at[slot, i])
                for i, (s, d) in enumerate(((eg, wg), (eu, wu), (ed, wd)))]

    h_copy = pltpu.make_async_copy(h_hbm, hv.at[pl.ds(0, n_tok)], h_sem)
    s_copy = pltpu.make_async_copy(sum_hbm, acc.at[pl.ds(0, n_tok)], s_sem)
    h_copy.start()
    s_copy.start()
    routing(idx_ref, lax.axis_index("ep") * n_local, n_tok, n_local, n_row, pos_v, list_v, x4, y4)
    l_copy = pltpu.make_async_copy(list_v, list_ref, l_sem)
    l_copy.start()
    l_copy.wait()

    def exp_tiles(e):
        return list_ref[n_row + e, 0]

    def fill(e, t):
        def put(j, _):
            tile_exp[t + j] = e
            return 0
        count = exp_tiles(e)
        lax.fori_loop(0, count, put, 0)
        return t + count
    n_tile = lax.fori_loop(0, n_local, fill, 0)

    @pl.when(n_tile > 0)
    def _():
        for c in weight_copies(tile_exp[0], 0):
            c.start()
    h_copy.wait()

    def gather(base, g):
        for u in range(GROUP):
            i = g * GROUP + u
            tok = list_ref[base * span + i // LANES, i % LANES] & TOK_MASK
            x4[pl.ds(i, chunks, stride=PITCH), :] = hv[tok].astype(jnp.float32)

    def pack(k):
        xb[:, k * LANES:(k + 1) * LANES] = x4[k * PITCH:k * PITCH + TILE, :].astype(jnp.bfloat16)

    def scatter(base, g):
        sums = []
        for u in range(GROUP):
            i = g * GROUP + u
            entry = list_ref[base * span + i // LANES, i % LANES]
            tok = entry & TOK_MASK
            sums.append((tok, acc[tok] + y4[pl.ds(i, chunks, stride=PITCH), :] * wt_ref[entry]))
        for tok, v in sums:
            acc[tok] = v

    def loop(fn, base):
        def body(g, _):
            fn(base, g)
            return 0
        lax.fori_loop(0, TILE // GROUP, body, 0)

    loop(gather, 0)
    for k in range(chunks):
        pack(k)
    def tile(t, slot):
        e = tile_exp[t]
        fresh = (t == 0) | (e != tile_exp[jnp.maximum(t - 1, 0)])
        slot = jnp.where(fresh, 1 - slot, slot)

        @pl.when(fresh)
        def _():
            for c in weight_copies(e, slot):
                c.wait()
            after = t + exp_tiles(e)

            @pl.when(after < n_tile)
            def _():
                for c in weight_copies(tile_exp[after], 1 - slot):
                    c.start()

        @pl.when(t == 1)
        def _():
            s_copy.wait()

        prev = jnp.where(t == 0, last, t - 1)
        n_group = TILE // GROUP
        gate = dot_t(xb[...], wg[slot])
        up = dot_t(xb[...], wu[slot])
        for g in range(n_group):
            scatter(prev, g)
        act[...] = (jax.nn.silu(gate) * up).astype(jnp.bfloat16)
        for g in range(n_group):
            gather(t + 1, g)
        for k in range(0, chunks, 2):
            d = jnp.dot(act[...], wd[slot, :, k * LANES:(k + 2) * LANES], preferred_element_type=jnp.float32)
            y4[k * PITCH:k * PITCH + TILE, :] = d[:, :LANES]
            y4[(k + 1) * PITCH:(k + 1) * PITCH + TILE, :] = d[:, LANES:]
        for k in range(chunks):
            pack(k)
        return slot

    lax.fori_loop(0, n_tile, tile, 1)

    @pl.when(n_tile <= 1)
    def _():
        s_copy.wait()
    loop(scatter, jnp.where(n_tile == 0, last, n_tile - 1))

    blk = 256

    def flush(i, _):
        def conv(j, _):
            r = i * blk + j * 16
            hv[pl.ds(r, 16)] = acc[pl.ds(r, 16)].astype(jnp.bfloat16)
            return 0
        lax.fori_loop(0, blk // 16, conv, 0)
        pltpu.make_async_copy(hv.at[pl.ds(i * blk, blk)], out_hbm.at[pl.ds(i * blk, blk)], o_sem).start()
        return 0
    lax.fori_loop(0, n_tok // blk, flush, 0)
    pltpu.make_async_copy(hv.at[pl.ds(0, n_tok)], out_hbm, o_sem).wait()


def moe(idx, wt, h3, sums, eg, eu, ed):
    n_tok, chunks, _ = h3.shape
    hidden = chunks * LANES
    width = ed.shape[1]
    smem = pl.BlockSpec(memory_space=pltpu.SMEM)
    hbm = pl.BlockSpec(memory_space=pl.ANY)
    max_tiles = -(-(idx.size + eg.shape[0] * (TILE - 1)) // TILE) + 1
    n_row = -(-max_tiles * TILE // (16 * LANES)) * 16
    return pl.pallas_call(
        moe_kernel,
        out_shape=jax.ShapeDtypeStruct((n_tok, chunks, LANES), jnp.bfloat16),
        in_specs=[pl.BlockSpec(memory_space=pltpu.VMEM), smem] + [hbm] * 5,
        out_specs=hbm,
        scratch_shapes=[
            pltpu.VMEM((n_tok + GROUP, chunks, LANES), jnp.bfloat16),
            pltpu.VMEM((n_tok + GROUP, chunks, LANES), jnp.float32),
            pltpu.VMEM((2, width, hidden), jnp.bfloat16),
            pltpu.VMEM((2, width, hidden), jnp.bfloat16),
            pltpu.VMEM((2, width, hidden), jnp.bfloat16),
            pltpu.VMEM((chunks * PITCH + 8, LANES), jnp.float32),
            pltpu.VMEM((TILE, hidden), jnp.bfloat16),
            pltpu.VMEM((TILE, width), jnp.bfloat16),
            pltpu.VMEM((chunks * PITCH + 8, LANES), jnp.float32),
            pltpu.VMEM(idx.shape, jnp.int32),
            pltpu.VMEM((n_row + 16, LANES), jnp.int32),
            pltpu.SMEM((n_row + 16, LANES), jnp.int32),
            pltpu.SMEM((max_tiles + 1,), jnp.int32),
            pltpu.SemaphoreType.DMA,
            pltpu.SemaphoreType.DMA,
            pltpu.SemaphoreType.DMA((2, 3)),
            pltpu.SemaphoreType.DMA,
            pltpu.SemaphoreType.DMA,
        ],
        compiler_params=pltpu.CompilerParams(vmem_limit_bytes=67043328),
        cost_estimate=pl.CostEstimate(flops=2 * 3 * hidden * width * n_tok, bytes_accessed=130_000_000, transcendentals=0),
        name="moe",
    )(idx, wt, h3, sums, eg, eu, ed)


def front_kernel(hid, gain_ref, head_ref, sig_ref, idx_ref, sg, su, sd, h_out, sum_out, wt_out,
                 hbuf, x4, xb, act, y4, stage, t4, h_sem, s_sem, pair_send, pair_recv, y_send, y_recv, z_send, z_recv,
                 fwd_send, fwd_recv):
    z, e = lax.axis_index("tp"), lax.axis_index("ep")
    rows, hidden = hid.shape
    chunks = hidden // LANES
    size = t4.shape[0] // chunks - 1
    n_chunk = rows // (2 * size)
    core = e % 2
    pair = e + 1 - 2 * core
    far = (e + 2) % 4
    far_pair = (pair + 2) % 4
    half = z % 2
    zpair = z + 1 - 2 * half

    barrier = pltpu.get_barrier_semaphore()
    for dev in ({"ep": pair}, {"ep": far}, {"tp": zpair}):
        pl.semaphore_signal(barrier, inc=1, device_id=dev, device_id_type=MESH)
    pl.semaphore_wait(barrier, 3)

    def send_rows(block, h, j):
        return hbuf.at[pl.ds(block * rows + h * (rows // 2) + j * size, size)]

    def y_copy(j):
        mine = send_rows(e, half, j)
        return pltpu.make_async_remote_copy(mine, mine, y_send.at[j], y_recv.at[j], device_id={"ep": far}, device_id_type=MESH)

    def z_copy(j):
        got = send_rows(far, half, j)
        return pltpu.make_async_remote_copy(got, got, z_send.at[j], z_recv.at[j], device_id={"tp": zpair}, device_id_type=MESH)

    def fwd_copy(j, side):
        got = send_rows(far, half if side == 0 else 1 - half, j)
        return pltpu.make_async_remote_copy(
            got, got, fwd_send.at[side, j], fwd_recv.at[side, j], device_id={"ep": pair}, device_id_type=MESH)

    own = hbuf.at[pl.ds(e * rows, rows)]
    to_pair = pltpu.make_async_remote_copy(own, own, pair_send, pair_recv, device_id={"ep": pair}, device_id_type=MESH)
    gain = gain_ref[...].astype(jnp.float32)

    def norm(c, _):
        lo = (half * n_chunk + c) % (2 * n_chunk) * size
        x = hid[pl.ds(lo, size), :].astype(jnp.float32)
        inv_rms = lax.rsqrt(jnp.mean(x * x, axis=-1, keepdims=True) + RMS_EPS)
        h = (x * inv_rms * gain).astype(jnp.bfloat16).astype(jnp.float32)
        for k in range(chunks):
            t4[k * (size + 1):k * (size + 1) + size, :] = h[:, k * LANES:(k + 1) * LANES]
        for i in range(size):
            hbuf[e * rows + lo + i] = t4[pl.ds(i, chunks, stride=size + 1), :].astype(jnp.bfloat16)

        @pl.when(c < n_chunk)
        def _():
            y_copy(c).start()
        return 0
    lax.fori_loop(0, 2 * n_chunk, norm, 0)
    to_pair.start()

    def relay_y(j):
        y_copy(j).wait_recv()
        z_copy(j).start()
        fwd_copy(j, 0).start()

    def relay_z(j):
        z_copy(j).wait_recv()
        fwd_copy(j, 1).start()

    n_tile = 4 * rows // TILE
    per = rows // TILE
    quarter = n_chunk // 2
    half_step, flight = 1.7, 45.0 / n_chunk
    due = {}
    for j in range(n_chunk):
        y_at = 5 + flight * (j + 1)
        for kind, at_time, need in (("y", y_at, 16 if j < quarter else 24), ("z", y_at + flight + 3, 20 if j < quarter else 28)):
            q = min(need, max(0, math.ceil((at_time - 5) / half_step)))
            due.setdefault(q, []).append((at_time, kind, j))
    due.setdefault(8, []).append((0, "p", 0))
    for q, kind, j in ((18, "a", 0), (22, "b", 0), (26, "a", 1), (30, "b", 1)):
        due.setdefault(q, []).append((1e3, kind, j))

    def h_rows(base):
        return pltpu.make_async_copy(hbuf.at[pl.ds(base, TILE)], h_out.at[pl.ds(base, TILE)], h_sem)

    def do(what):
        _, kind, arg = what
        if kind == "p":
            to_pair.wait_recv()
        elif kind == "y":
            relay_y(arg)
        elif kind == "z":
            relay_z(arg)
        else:
            for j in range(quarter):
                fwd_copy(arg * quarter + j, 0 if kind == "a" else 1).wait_recv()

    def sum_copy(base, slot):
        return pltpu.make_async_copy(stage.at[slot], sum_out.at[pl.ds(base, TILE)], s_sem.at[slot])

    sig = sig_ref[...].astype(jnp.float32)

    def relay(q, parity):
        for at_step, what in due.items():
            if at_step % 2 == parity:
                @pl.when(q == at_step)
                def _(what=what):
                    for w in sorted(what):
                        do(w)

    def tile(s, _):
        relay(2 * s, 0)
        u = s - 2 * per
        near = s // per
        near_block = e + near * (pair - e)
        near_base = near_block * rows + s % per * TILE
        far_block = far + u % 2 * (far_pair - far)
        far_half = half + u // 2 % 2 * (1 - 2 * half)
        far_base = far_block * rows + far_half * (rows // 2) + u // 4 * TILE
        is_far = s // (2 * per)
        base = pl.multiple_of(near_base + is_far * (far_base - near_base), TILE)
        block = near_block + is_far * (far_block - near_block)
        col = pl.multiple_of(base - block * rows, TILE)
        slot = s % 2

        def fill(g, _):
            for v in range(16):
                i = g * 16 + v
                x4[pl.ds(i, chunks, stride=PITCH), :] = hbuf[base + i].astype(jnp.float32)
            return 0
        lax.fori_loop(0, TILE // 16, fill, 0)
        for k in range(chunks):
            xb[:, k * LANES:(k + 1) * LANES] = x4[k * PITCH:k * PITCH + TILE, :].astype(jnp.bfloat16)

        logits = dot_t(head_ref[...], xb[...])
        prob = jnp.exp(logits - jnp.max(logits, axis=0, keepdims=True))
        prob = prob / jnp.sum(prob, axis=0, keepdims=True)
        expert = lax.broadcasted_iota(jnp.int32, prob.shape, 0)
        idx = idx_ref[block, :, pl.ds(col, TILE)]
        picked = [jnp.sum(jnp.where(expert == idx[k:k + 1, :], prob, 0.0), axis=0, keepdims=True) for k in range(idx.shape[0])]
        wt_out[:, pl.ds(base, TILE)] = jnp.concatenate(picked, axis=0)

        gate = dot_t(xb[...], sg[...])
        up = dot_t(xb[...], su[...])
        act[...] = (jax.nn.silu(gate) * up).astype(jnp.bfloat16)
        scale = jax.nn.sigmoid(jnp.sum(xb[...].astype(jnp.float32) * sig, axis=1, keepdims=True))
        for k in range(0, chunks, 2):
            d = jnp.dot(act[...], sd[:, k * LANES:(k + 2) * LANES], preferred_element_type=jnp.float32) * scale
            y4[k * PITCH:k * PITCH + TILE, :] = d[:, :LANES]
            y4[(k + 1) * PITCH:(k + 1) * PITCH + TILE, :] = d[:, LANES:]

        relay(2 * s + 1, 1)
        h_rows(base).start()

        @pl.when(s >= 2)
        def _():
            sum_copy(0, slot).wait()

        def put(g, _):
            for v in range(16):
                i = g * 16 + v
                stage[slot, i] = y4[pl.ds(i, chunks, stride=PITCH), :]
            return 0
        lax.fori_loop(0, TILE // 16, put, 0)
        sum_copy(base, slot).start()
        return 0
    lax.fori_loop(0, n_tile, tile, 0)

    def drain(j, _):
        fwd_copy(j, 0).wait_send()
        fwd_copy(j, 1).wait_send()
        y_copy(j).wait_send()
        z_copy(j).wait_send()
        return 0
    lax.fori_loop(0, n_chunk, drain, 0)
    to_pair.wait_send()
    pltpu.make_async_copy(hbuf, h_out, h_sem).wait()
    sum_copy(0, 0).wait()
    sum_copy(0, 1).wait()


def front(hidden_in, gain, head, sig, all_idx, sg, su, sd):
    rows, hidden = hidden_in.shape
    ranks, n_top, _ = all_idx.shape
    width = sg.shape[0]
    chunks = hidden // LANES
    n_tok = ranks * rows
    size = rows // (2 * SPREAD_CHUNKS)
    dma = pltpu.SemaphoreType.DMA
    vmem = pl.BlockSpec(memory_space=pltpu.VMEM)
    hbm = pl.BlockSpec(memory_space=pl.ANY)
    pitched = pltpu.VMEM((chunks * PITCH + 8, LANES), jnp.float32)
    return pl.pallas_call(
        front_kernel,
        out_shape=(jax.ShapeDtypeStruct((n_tok, chunks, LANES), jnp.bfloat16),
                   jax.ShapeDtypeStruct((n_tok, chunks, LANES), jnp.float32),
                   jax.ShapeDtypeStruct((n_top, TOK_MASK + 1), jnp.float32)),
        in_specs=[vmem] * 8,
        out_specs=(hbm, hbm, vmem),
        scratch_shapes=[
            pltpu.VMEM((n_tok, chunks, LANES), jnp.bfloat16), pitched, pltpu.VMEM((TILE, hidden), jnp.bfloat16),
            pltpu.VMEM((TILE, width), jnp.bfloat16), pitched, pltpu.VMEM((2, TILE, chunks, LANES), jnp.float32),
            pltpu.VMEM((chunks * (size + 1), LANES), jnp.float32),
            dma, dma((2,)), dma, dma] + [dma((SPREAD_CHUNKS,))] * 4 + [dma((2, SPREAD_CHUNKS))] * 2,
        compiler_params=pltpu.CompilerParams(collective_id=0, has_side_effects=True, vmem_limit_bytes=60 << 20),
        name="front",
    )(hidden_in, gain, head, sig, all_idx, sg, su, sd)


def combine_kernel(n_chunk, lag, part, hid_hbm, out_ref, mine, near, far_in, zin, hid, t4, m_sem, h_sem,
                   d_send, d_recv, y_send, y_recv, z_send, z_recv, t_send):
    z, e = lax.axis_index("tp"), lax.axis_index("ep")
    rows = out_ref.shape[0]
    chunks = part.shape[1]
    size = rows // n_chunk
    core = e % 2
    pair = e + 1 - 2 * core
    far = (e + 2) % 4
    far_pair = (pair + 2) % 4
    n_z = 4
    zn = z + 1 - 2 * (z % 2)

    barrier = pltpu.get_barrier_semaphore()
    for dev in ({"ep": pair}, {"ep": far}):
        pl.semaphore_signal(barrier, inc=1, device_id=dev, device_id_type=MESH)

    @pl.when(z > 0)
    def _():
        pl.semaphore_signal(barrier, inc=1, device_id={"tp": z - 1}, device_id_type=MESH)

    @pl.when(z < n_z - 1)
    def _():
        pl.semaphore_signal(barrier, inc=1, device_id={"tp": z + 1}, device_id_type=MESH)
    at_end = (z == 0) | (z == n_z - 1)

    @pl.when(at_end)
    def _():
        pl.semaphore_wait(barrier, 3)

    @pl.when(jnp.logical_not(at_end))
    def _():
        pl.semaphore_wait(barrier, 4)

    def at(j):
        return pl.ds(j * size, size)

    def d_copy(j, side):
        owner = far_pair if side == 0 else pair
        return pltpu.make_async_remote_copy(
            part.at[pl.ds(owner * rows + j * size, size)], near.at[side, at(j)],
            d_send.at[side, j], d_recv.at[side, j], device_id={"ep": pair}, device_id_type=MESH)

    def m_copy(j, side):
        owner = far if side == 0 else e
        return pltpu.make_async_copy(part.at[pl.ds(owner * rows + j * size, size)], mine.at[side, at(j)], m_sem.at[side, j])

    def y_copy(j):
        return pltpu.make_async_remote_copy(
            mine.at[0, at(j)], far_in.at[at(j)], y_send.at[j], y_recv.at[j], device_id={"ep": far}, device_id_type=MESH)

    def z_copy(j, slot, to):
        return pltpu.make_async_remote_copy(
            mine.at[1, at(j)], zin.at[slot, at(j)], z_send.at[j], z_recv.at[slot, j], device_id={"tp": to}, device_id_type=MESH)

    def t_copy(j, side, to, src):
        return pltpu.make_async_remote_copy(
            src, zin.at[1, at(j)], t_send.at[side, j], z_recv.at[1, j], device_id={"tp": to}, device_id_type=MESH)

    hid_copy = pltpu.make_async_copy(hid_hbm, hid, h_sem)

    def first(j, _):
        for side in range(2):
            d_copy(j, side).start()
            m_copy(j, side).start()
        return 0
    lax.fori_loop(0, n_chunk, first, 0)
    hid_copy.start()

    def f32(ref):
        return ref[...].astype(jnp.float32)

    def finish(j, src):
        def put(g, _):
            for u in range(8):
                i = g * 8 + u
                t4[pl.ds(i, chunks, stride=size + 1), :] = src[i].astype(jnp.float32)
            return 0
        lax.fori_loop(0, size // 8, put, 0)
        for k in range(chunks):
            cols = slice(k * LANES, (k + 1) * LANES)
            tot = t4[k * (size + 1):k * (size + 1) + size, :]
            out_ref[at(j), cols] = (hid[at(j), cols].astype(jnp.float32) + tot).astype(jnp.bfloat16)

    def step(i, _):
        @pl.when(i < n_chunk)
        def _():
            for side in range(2):
                d_copy(i, side).wait_recv()
                m_copy(i, side).wait()
            mine[0, at(i)] = (f32(mine.at[0, at(i)]) + f32(near.at[0, at(i)])).astype(jnp.bfloat16)
            y_copy(i).start()

        def stage(shift):
            j = i - shift * lag
            odd = j % 2
            spot = z + odd * (n_z - 1 - 2 * z)
            ahead = 1 - 2 * odd
            return j, spot, ahead, (j >= 0) & (j < n_chunk)

        @pl.when(i == 3 * lag)
        def _():
            hid_copy.wait()

        j, spot, ahead, live = stage(1)

        @pl.when(live)
        def _():
            y_copy(j).wait_recv()
            mine[1, at(j)] = (f32(mine.at[1, at(j)]) + f32(near.at[1, at(j)]) + f32(far_in.at[at(j)])).astype(jnp.bfloat16)

            @pl.when(spot == 0)
            def _():
                z_copy(j, 0, z + ahead).start()

            @pl.when(spot == 3)
            def _():
                z_copy(j, 0, z - ahead).start()

        j2, spot2, ahead2, live2 = stage(2)

        @pl.when(live2 & (spot2 == 2))
        def _():
            z_copy(j2, 0, zn).wait_recv()
            mine[1, at(j2)] = (f32(mine.at[1, at(j2)]) + f32(zin.at[0, at(j2)])).astype(jnp.bfloat16)
            z_copy(j2, 1, z - ahead2).start()

        j3, spot3, ahead3, live3 = stage(3)

        @pl.when(live3 & (spot3 == 1))
        def _():
            z_copy(j3, 0, zn).wait_recv()
            z_copy(j3, 1, zn).wait_recv()
            mine[1, at(j3)] = (f32(mine.at[1, at(j3)]) + f32(zin.at[0, at(j3)]) + f32(zin.at[1, at(j3)])).astype(jnp.bfloat16)
            t_copy(j3, 0, z - ahead3, mine.at[1, at(j3)]).start()
            t_copy(j3, 1, z + ahead3, mine.at[1, at(j3)]).start()
            finish(j3, mine.at[1, at(j3)])

        j4, spot4, ahead4, live4 = stage(4)

        @pl.when(live4 & (spot4 == 2))
        def _():
            z_copy(j4, 1, zn).wait_recv()
            t_copy(j4, 0, z + ahead4, zin.at[1, at(j4)]).start()
            finish(j4, zin.at[1, at(j4)])

        j5, spot5, ahead5, live5 = stage(5)

        @pl.when(live5 & ((spot5 == 0) | (spot5 == 3)))
        def _():
            z_copy(j5, 1, zn).wait_recv()
            finish(j5, zin.at[1, at(j5)])
        return 0
    lax.fori_loop(0, n_chunk + 5 * lag, step, 0)

    def drain(j, _):
        odd = j % 2
        spot = z + odd * (n_z - 1 - 2 * z)
        d_copy(j, 0).wait_send()
        d_copy(j, 1).wait_send()
        y_copy(j).wait_send()

        @pl.when(spot != 1)
        def _():
            z_copy(j, 0, zn).wait_send()

        @pl.when((spot == 1) | (spot == 2))
        def _():
            t_copy(j, 0, zn, mine.at[1, at(j)]).wait_send()

        @pl.when(spot == 1)
        def _():
            t_copy(j, 1, zn, mine.at[1, at(j)]).wait_send()
        return 0
    lax.fori_loop(0, n_chunk, drain, 0)


def combine(part, hidden_in, n_chunk, lag):
    rows, hidden = hidden_in.shape
    block = (rows,) + part.shape[1:]
    dma = pltpu.SemaphoreType.DMA
    size = rows // n_chunk
    hbm = pl.BlockSpec(memory_space=pl.ANY)
    return pl.pallas_call(
        functools.partial(combine_kernel, n_chunk, lag),
        out_shape=jax.ShapeDtypeStruct((rows, hidden), jnp.bfloat16),
        in_specs=[hbm, hbm],
        out_specs=pl.BlockSpec(memory_space=pltpu.VMEM),
        scratch_shapes=[
            pltpu.VMEM((2,) + block, jnp.bfloat16), pltpu.VMEM((2,) + block, jnp.bfloat16), pltpu.VMEM(block, jnp.bfloat16),
            pltpu.VMEM((2,) + block, jnp.bfloat16), pltpu.VMEM((rows, hidden), jnp.bfloat16),
            pltpu.VMEM(((size + 1) * part.shape[1] + 8, LANES), jnp.float32),
            dma((2, n_chunk)), dma, dma((2, n_chunk)), dma((2, n_chunk)), dma((n_chunk,)), dma((n_chunk,)),
            dma((n_chunk,)), dma((2, n_chunk)), dma((2, n_chunk)),
        ],
        compiler_params=pltpu.CompilerParams(collective_id=1, has_side_effects=True, vmem_limit_bytes=60 << 20),
        name="combine",
    )(part, hidden_in)


def solution(mesh):
    tok_spec = P(('dp', 'ep'), None)
    in_specs = (tok_spec, tok_spec, P(None), P(None, None), P(None, None),
                P('ep', None, 'tp'), P('ep', None, 'tp'), P('ep', 'tp', None),
                P(None, ('tp', 'ep')), P(None, ('tp', 'ep')), P(('tp', 'ep'), None))

    def local_step(hidden_in, topk_idx, norm_gain, router_w, shared_sig_w, exp_gate, exp_up, exp_down, sh_gate, sh_up, sh_down):
        all_idx = lax.all_gather(topk_idx.T, 'ep', axis=0)
        all_h, sums, wt = front(hidden_in, norm_gain[None, :], router_w.T, shared_sig_w.T, all_idx, sh_gate.T, sh_up.T, sh_down)
        by_top = jnp.swapaxes(all_idx, 0, 1).reshape(-1, LANES)
        part = moe(by_top, wt.reshape(-1), all_h, sums, jnp.swapaxes(exp_gate, 1, 2), jnp.swapaxes(exp_up, 1, 2), exp_down)
        return combine(part, hidden_in, COMBINE_CHUNKS, COMBINE_LAG)

    return jax.shard_map(local_step, mesh=mesh, in_specs=in_specs, out_specs=tok_spec, check_vma=False)
```

```python
import functools
import math

import jax
import jax.numpy as jnp
from jax import lax
from jax.experimental import pallas as pl
from jax.experimental.pallas import tpu as pltpu
from jax.sharding import PartitionSpec as P

RMS_EPS = 1e-6
LANES = 128
TILE = 256
PITCH = TILE + 1
GROUP = 8
TOK_MASK = 8191
MESH = pl.DeviceIdType.MESH
SPREAD_CHUNKS = 16
COMBINE_CHUNKS = 64
COMBINE_LAG = 3


def dot_t(a, b):
    return lax.dot_general(a, b, (((1,), (1,)), ((), ())), preferred_element_type=jnp.float32)


def routing(idx_ref, first, ranks, n_tok, n_local, n_row, pos_v, list_v, in_row, totals):
    n = idx_ref.shape[0]
    i32, bf16, f32 = jnp.int32, jnp.bfloat16, jnp.float32
    sub = lax.broadcasted_iota(i32, (LANES, LANES), 0)
    lane = lax.broadcasted_iota(i32, (LANES, LANES), 1)
    below = jnp.where(sub < lane, 1.0, 0.0).astype(bf16)
    above = jnp.where(lane < sub, 1.0, 0.0).astype(bf16)
    ones = jnp.ones((LANES, LANES), bf16)

    def mask(e):
        return jnp.where(idx_ref[...] == first + e, 1.0, 0.0)

    both = jnp.concatenate([below, ones], axis=1)
    for e in range(n_local):
        got = jnp.dot(mask(e).astype(bf16), both, preferred_element_type=f32)
        in_row[e * n:(e + 1) * n, :] = got[:, :LANES]
        totals[e * n:(e + 1) * n, :] = got[:, LANES:]
    pos = jnp.zeros((n, LANES), f32)
    start = jnp.zeros((1, LANES), i32)
    for e in range(n_local):
        total = totals[e * n:(e + 1) * n, :]
        before = jnp.dot(above, total.astype(bf16), preferred_element_type=f32)
        count = (before[n - 1:n] + total[n - 1:n]).astype(i32)
        tiles = (count + TILE - 1) // TILE
        list_v[n_row + e:n_row + e + 1, :] = tiles
        pos += mask(e) * (in_row[e * n:(e + 1) * n, :] + before + (start * TILE).astype(f32) + 1.0)
        start += tiles
    pos_v[...] = pos.astype(i32) - 1

    rows = lax.broadcasted_iota(i32, (n_row, LANES), 0)
    step = 8
    nb = n_tok // ranks // LANES
    n_top = n * LANES // n_tok
    base = n_tok // LANES
    lane_val = lax.broadcasted_iota(i32, (LANES, LANES), 1).astype(f32)

    def add(g, acc):
        lhs, rhs = [], []
        for u in range(step):
            r = g * step + u
            p = pos_v[pl.ds(r, 1), :]
            tok_row = r // (nb * n_top) * nb + r % nb
            code = (r // nb % n_top * ((TOK_MASK + 1) // LANES) + tok_row - base).astype(f32)
            lhs.append(jnp.where(rows == p // LANES, 1.0, 0.0).astype(bf16))
            hit = sub == jnp.where(p < 0, LANES, p % LANES)
            rhs.append(jnp.concatenate([jnp.where(hit, code, 0.0), jnp.where(hit, lane_val, 0.0)], axis=0).astype(bf16))
        return acc + dot_t(jnp.concatenate(lhs, axis=1), jnp.concatenate(rhs, axis=1))
    acc = lax.fori_loop(0, n // step, add, jnp.zeros((n_row, 2 * LANES), f32))
    list_v[0:n_row, :] = (acc[:, :LANES] * LANES + acc[:, LANES:]).astype(i32) + n_tok


def moe_kernel(idx_ref, wt_hbm, h_hbm, sum_hbm, eg, eu, ed, out_hbm,
               hv, acc, wg, wu, wd, x4, xb, act, y4, pos_v, list_v, list_ref, tile_exp, wt_ref, h_sem, s_sem, w_sem, o_sem, l_sem, t_sem):
    n_tok, chunks, _ = h_hbm.shape
    n_local, width, _ = ed.shape
    n_row = list_v.shape[0] - 16
    span = TILE // LANES
    last = n_row // span - 1

    def weight_copies(e, slot):
        return [pltpu.make_async_copy(s.at[e], d.at[slot], w_sem.at[slot, i])
                for i, (s, d) in enumerate(((eg, wg), (eu, wu), (ed, wd)))]

    h_copy = pltpu.make_async_copy(h_hbm, hv.at[pl.ds(0, n_tok)], h_sem)
    s_copy = pltpu.make_async_copy(sum_hbm, acc.at[pl.ds(0, n_tok)], s_sem)
    t_copy = pltpu.make_async_copy(wt_hbm, wt_ref, t_sem)
    h_copy.start()
    t_copy.start()
    s_copy.start()
    routing(idx_ref, lax.axis_index("ep") * n_local, lax.axis_size("ep"), n_tok, n_local, n_row, pos_v, list_v, x4, y4)
    l_copy = pltpu.make_async_copy(list_v, list_ref, l_sem)
    l_copy.start()
    l_copy.wait()

    def exp_tiles(e):
        return list_ref[n_row + e, 0]

    def fill(e, t):
        def put(j, _):
            tile_exp[t + j] = e
            return 0
        count = exp_tiles(e)
        lax.fori_loop(0, count, put, 0)
        return t + count
    n_tile = lax.fori_loop(0, n_local, fill, 0)

    @pl.when(n_tile > 0)
    def _():
        for c in weight_copies(tile_exp[0], 0):
            c.start()
    h_copy.wait()
    t_copy.wait()

    def gather(base, g):
        for u in range(GROUP):
            i = g * GROUP + u
            tok = list_ref[base * span + i // LANES, i % LANES] & TOK_MASK
            x4[pl.ds(i, chunks, stride=PITCH), :] = hv[tok].astype(jnp.float32)

    def pack(k):
        xb[:, k * LANES:(k + 1) * LANES] = x4[k * PITCH:k * PITCH + TILE, :].astype(jnp.bfloat16)

    def scatter(base, g):
        sums = []
        for u in range(GROUP):
            i = g * GROUP + u
            entry = list_ref[base * span + i // LANES, i % LANES]
            tok = entry & TOK_MASK
            sums.append((tok, acc[tok] + y4[pl.ds(i, chunks, stride=PITCH), :] * wt_ref[entry]))
        for tok, v in sums:
            acc[tok] = v

    def loop(fn, base):
        for g in range(TILE // GROUP):
            fn(base, g)

    loop(gather, 0)
    for k in range(chunks):
        pack(k)
    def tile(t, slot):
        e = tile_exp[t]
        fresh = (t == 0) | (e != tile_exp[jnp.maximum(t - 1, 0)])
        slot = jnp.where(fresh, 1 - slot, slot)

        @pl.when(fresh)
        def _():
            for c in weight_copies(e, slot):
                c.wait()
            after = t + exp_tiles(e)

            @pl.when(after < n_tile)
            def _():
                for c in weight_copies(tile_exp[after], 1 - slot):
                    c.start()

        @pl.when(t == 1)
        def _():
            s_copy.wait()

        prev = jnp.where(t == 0, last, t - 1)
        n_group = TILE // GROUP
        gate = dot_t(xb[...], wg[slot])
        up = dot_t(xb[...], wu[slot])
        for g in range(n_group):
            scatter(prev, g)
        act[...] = (jax.nn.silu(gate) * up).astype(jnp.bfloat16)
        for g in range(n_group):
            gather(t + 1, g)
        for k in range(0, chunks, 2):
            d = jnp.dot(act[...], wd[slot, :, k * LANES:(k + 2) * LANES], preferred_element_type=jnp.float32)
            y4[k * PITCH:k * PITCH + TILE, :] = d[:, :LANES]
            y4[(k + 1) * PITCH:(k + 1) * PITCH + TILE, :] = d[:, LANES:]
        for k in range(chunks):
            pack(k)
        return slot

    lax.fori_loop(0, n_tile, tile, 1)

    @pl.when(n_tile <= 1)
    def _():
        s_copy.wait()
    loop(scatter, jnp.where(n_tile == 0, last, n_tile - 1))

    blk = 256

    def flush(i, _):
        def conv(j, _):
            r = i * blk + j * 16
            hv[pl.ds(r, 16)] = acc[pl.ds(r, 16)].astype(jnp.bfloat16)
            return 0
        lax.fori_loop(0, blk // 16, conv, 0)
        pltpu.make_async_copy(hv.at[pl.ds(i * blk, blk)], out_hbm.at[pl.ds(i * blk, blk)], o_sem).start()
        return 0
    lax.fori_loop(0, n_tok // blk, flush, 0)
    pltpu.make_async_copy(hv.at[pl.ds(0, n_tok)], out_hbm, o_sem).wait()


def moe(idx, wt, h3, sums, eg, eu, ed):
    n_tok, chunks, _ = h3.shape
    hidden = chunks * LANES
    width = ed.shape[1]
    hbm = pl.BlockSpec(memory_space=pl.ANY)
    max_tiles = -(-(idx.size + eg.shape[0] * (TILE - 1)) // TILE) + 1
    n_row = -(-max_tiles * TILE // (16 * LANES)) * 16
    return pl.pallas_call(
        moe_kernel,
        out_shape=jax.ShapeDtypeStruct((n_tok, chunks, LANES), jnp.bfloat16),
        in_specs=[pl.BlockSpec(memory_space=pltpu.VMEM)] + [hbm] * 6,
        out_specs=hbm,
        scratch_shapes=[
            pltpu.VMEM((n_tok + GROUP, chunks, LANES), jnp.bfloat16),
            pltpu.VMEM((n_tok + GROUP, chunks, LANES), jnp.float32),
            pltpu.VMEM((2, width, hidden), jnp.bfloat16),
            pltpu.VMEM((2, width, hidden), jnp.bfloat16),
            pltpu.VMEM((2, width, hidden), jnp.bfloat16),
            pltpu.VMEM((chunks * PITCH + 8, LANES), jnp.float32),
            pltpu.VMEM((TILE, hidden), jnp.bfloat16),
            pltpu.VMEM((TILE, width), jnp.bfloat16),
            pltpu.VMEM((chunks * PITCH + 8, LANES), jnp.float32),
            pltpu.VMEM(idx.shape, jnp.int32),
            pltpu.VMEM((n_row + 16, LANES), jnp.int32),
            pltpu.SMEM((n_row + 16, LANES), jnp.int32),
            pltpu.SMEM((max_tiles + 1,), jnp.int32),
            pltpu.SMEM(wt.shape, jnp.float32),
            pltpu.SemaphoreType.DMA,
            pltpu.SemaphoreType.DMA,
            pltpu.SemaphoreType.DMA((2, 3)),
            pltpu.SemaphoreType.DMA,
            pltpu.SemaphoreType.DMA,
            pltpu.SemaphoreType.DMA,
        ],
        compiler_params=pltpu.CompilerParams(vmem_limit_bytes=67043328),
        cost_estimate=pl.CostEstimate(flops=2 * 3 * hidden * width * n_tok, bytes_accessed=130_000_000, transcendentals=0),
        name="moe",
    )(idx, wt, h3, sums, eg, eu, ed)


def front_kernel(hid, gain_ref, head_ref, sig_ref, own_idx, sg, su, sd, h_out, sum_out, wt_out, idx_out,
                 idx_ref, wg, wu, wd, hbuf, x4, xb, act, y4, stage, t4, h_sem, s_sem, pair_send, pair_recv, y_send, y_recv, z_send, z_recv,
                 fwd_send, fwd_recv, w_sem, i_send, i_recv):
    z, e = lax.axis_index("tp"), lax.axis_index("ep")
    rows, hidden = hid.shape
    chunks = hidden // LANES
    size = t4.shape[0] // chunks - 1
    n_chunk = rows // (2 * size)
    core = e % 2
    pair = e + 1 - 2 * core
    far = (e + 2) % 4
    far_pair = (pair + 2) % 4
    half = z % 2
    zpair = z + 1 - 2 * half

    barrier = pltpu.get_barrier_semaphore()
    for dev in ({"ep": pair}, {"ep": far}, {"ep": far_pair}, {"tp": zpair}):
        pl.semaphore_signal(barrier, inc=1, device_id=dev, device_id_type=MESH)
    w_copies = [pltpu.make_async_copy(s, d, w_sem.at[i])
                for i, (s, d) in enumerate(((sg, wg), (su, wu), (sd, wd)))]
    for c in w_copies:
        c.start()
    pl.semaphore_wait(barrier, 4)

    i_copies = [pltpu.make_async_remote_copy(
        own_idx, idx_ref.at[e], i_send.at[i], i_recv.at[i], device_id={"ep": dev}, device_id_type=MESH)
        for i, dev in enumerate((pair, far, far_pair))]
    for c in i_copies:
        c.start()
    idx_ref[e] = own_idx[...]

    def send_rows(block, h, j):
        return hbuf.at[pl.ds(block * rows + h * (rows // 2) + j * size, size)]

    def y_copy(j):
        mine = send_rows(e, half, j)
        return pltpu.make_async_remote_copy(mine, mine, y_send.at[j], y_recv.at[j], device_id={"ep": far}, device_id_type=MESH)

    def z_copy(j):
        got = send_rows(far, half, j)
        return pltpu.make_async_remote_copy(got, got, z_send.at[j], z_recv.at[j], device_id={"tp": zpair}, device_id_type=MESH)

    def fwd_copy(j, side):
        got = send_rows(far, half if side == 0 else 1 - half, j)
        return pltpu.make_async_remote_copy(
            got, got, fwd_send.at[side, j], fwd_recv.at[side, j], device_id={"ep": pair}, device_id_type=MESH)

    own = hbuf.at[pl.ds(e * rows, rows)]
    to_pair = pltpu.make_async_remote_copy(own, own, pair_send, pair_recv, device_id={"ep": pair}, device_id_type=MESH)
    gain = gain_ref[...].astype(jnp.float32)

    def norm(c, _):
        lo = (half * n_chunk + c) % (2 * n_chunk) * size
        x = hid[pl.ds(lo, size), :].astype(jnp.float32)
        inv_rms = lax.rsqrt(jnp.mean(x * x, axis=-1, keepdims=True) + RMS_EPS)
        h = (x * inv_rms * gain).astype(jnp.bfloat16).astype(jnp.float32)
        for k in range(chunks):
            t4[k * (size + 1):k * (size + 1) + size, :] = h[:, k * LANES:(k + 1) * LANES]
        for i in range(size):
            hbuf[e * rows + lo + i] = t4[pl.ds(i, chunks, stride=size + 1), :].astype(jnp.bfloat16)

        @pl.when(c < n_chunk)
        def _():
            y_copy(c).start()
        return 0
    lax.fori_loop(0, 2 * n_chunk, norm, 0)
    to_pair.start()
    for c in w_copies:
        c.wait()

    def relay_y(j):
        y_copy(j).wait_recv()
        z_copy(j).start()
        fwd_copy(j, 0).start()

    def relay_z(j):
        z_copy(j).wait_recv()
        fwd_copy(j, 1).start()

    n_tile = 4 * rows // TILE
    per = rows // TILE
    quarter = n_chunk // 2
    half_step, flight = 1.7, 45.0 / n_chunk
    due = {}
    for j in range(n_chunk):
        y_at = 5 + flight * (j + 1)
        for kind, at_time, need in (("y", y_at, 16 if j < quarter else 24), ("z", y_at + flight + 3, 20 if j < quarter else 28)):
            q = min(need, max(0, math.ceil((at_time - 5) / half_step)))
            due.setdefault(q, []).append((at_time, kind, j))
    due.setdefault(8, []).append((0, "p", 0))
    for q, kind, j in ((18, "a", 0), (22, "b", 0), (26, "a", 1), (30, "b", 1)):
        due.setdefault(q, []).append((1e3, kind, j))

    def h_rows(base):
        return pltpu.make_async_copy(hbuf.at[pl.ds(base, TILE)], h_out.at[pl.ds(base, TILE)], h_sem)

    def do(what):
        _, kind, arg = what
        if kind == "p":
            to_pair.wait_recv()
            for c in i_copies:
                c.wait_recv()
            ranks, n_top, _ = idx_ref.shape
            nb = rows // LANES
            for r in range(ranks * n_top * nb):
                b = r % nb
                idx_out[r:r + 1, :] = idx_ref[r // (n_top * nb), r // nb % n_top:r // nb % n_top + 1, b * LANES:(b + 1) * LANES]
        elif kind == "y":
            relay_y(arg)
        elif kind == "z":
            relay_z(arg)
        else:
            for j in range(quarter):
                fwd_copy(arg * quarter + j, 0 if kind == "a" else 1).wait_recv()

    def sum_copy(base, slot):
        return pltpu.make_async_copy(stage.at[slot], sum_out.at[pl.ds(base, TILE)], s_sem.at[slot])

    sig = sig_ref[...].astype(jnp.float32)

    def relay(q, parity):
        for at_step, what in due.items():
            if at_step % 2 == parity:
                @pl.when(q == at_step)
                def _(what=what):
                    for w in sorted(what):
                        do(w)

    def tile(s, _):
        relay(2 * s, 0)
        u = s - 2 * per
        near = s // per
        near_block = e + near * (pair - e)
        near_base = near_block * rows + s % per * TILE
        far_block = far + u % 2 * (far_pair - far)
        far_half = half + u // 2 % 2 * (1 - 2 * half)
        far_base = far_block * rows + far_half * (rows // 2) + u // 4 * TILE
        is_far = s // (2 * per)
        base = pl.multiple_of(near_base + is_far * (far_base - near_base), TILE)
        block = near_block + is_far * (far_block - near_block)
        col = pl.multiple_of(base - block * rows, TILE)
        slot = s % 2

        def fill(g, _):
            for v in range(16):
                i = g * 16 + v
                x4[pl.ds(i, chunks, stride=PITCH), :] = hbuf[base + i].astype(jnp.float32)
            return 0
        lax.fori_loop(0, TILE // 16, fill, 0)
        for k in range(chunks):
            xb[:, k * LANES:(k + 1) * LANES] = x4[k * PITCH:k * PITCH + TILE, :].astype(jnp.bfloat16)

        logits = dot_t(head_ref[...], xb[...])
        prob = jnp.exp(logits - jnp.max(logits, axis=0, keepdims=True))
        prob = prob / jnp.sum(prob, axis=0, keepdims=True)
        expert = lax.broadcasted_iota(jnp.int32, prob.shape, 0)
        idx = idx_ref[block, :, pl.ds(col, TILE)]
        picked = [jnp.sum(jnp.where(expert == idx[k:k + 1, :], prob, 0.0), axis=0, keepdims=True) for k in range(idx.shape[0])]
        wt_out[:, pl.ds(base, TILE)] = jnp.concatenate(picked, axis=0)

        gate = dot_t(xb[...], wg[...])
        up = dot_t(xb[...], wu[...])
        act[...] = (jax.nn.silu(gate) * up).astype(jnp.bfloat16)
        scale = jax.nn.sigmoid(jnp.sum(xb[...].astype(jnp.float32) * sig, axis=1, keepdims=True))
        for k in range(0, chunks, 2):
            d = jnp.dot(act[...], wd[:, k * LANES:(k + 2) * LANES], preferred_element_type=jnp.float32) * scale
            y4[k * PITCH:k * PITCH + TILE, :] = d[:, :LANES]
            y4[(k + 1) * PITCH:(k + 1) * PITCH + TILE, :] = d[:, LANES:]

        relay(2 * s + 1, 1)
        h_rows(base).start()

        @pl.when(s >= 2)
        def _():
            sum_copy(0, slot).wait()

        def put(g, _):
            for v in range(16):
                i = g * 16 + v
                stage[slot, i] = y4[pl.ds(i, chunks, stride=PITCH), :]
            return 0
        lax.fori_loop(0, TILE // 16, put, 0)
        sum_copy(base, slot).start()
        return 0
    lax.fori_loop(0, n_tile, tile, 0)

    def drain(j, _):
        fwd_copy(j, 0).wait_send()
        fwd_copy(j, 1).wait_send()
        y_copy(j).wait_send()
        z_copy(j).wait_send()
        return 0
    lax.fori_loop(0, n_chunk, drain, 0)
    to_pair.wait_send()
    for c in i_copies:
        c.wait_send()
    pltpu.make_async_copy(hbuf, h_out, h_sem).wait()
    sum_copy(0, 0).wait()
    sum_copy(0, 1).wait()


def front(hidden_in, gain, head, sig, own_idx, ranks, sg, su, sd):
    rows, hidden = hidden_in.shape
    n_top = own_idx.shape[0]
    width = sg.shape[0]
    chunks = hidden // LANES
    n_tok = ranks * rows
    size = rows // (2 * SPREAD_CHUNKS)
    dma = pltpu.SemaphoreType.DMA
    vmem = pl.BlockSpec(memory_space=pltpu.VMEM)
    hbm = pl.BlockSpec(memory_space=pl.ANY)
    pitched = pltpu.VMEM((chunks * PITCH + 8, LANES), jnp.float32)
    return pl.pallas_call(
        front_kernel,
        out_shape=(jax.ShapeDtypeStruct((n_tok, chunks, LANES), jnp.bfloat16),
                   jax.ShapeDtypeStruct((n_tok, chunks, LANES), jnp.float32),
                   jax.ShapeDtypeStruct((n_top, TOK_MASK + 1), jnp.float32),
                   jax.ShapeDtypeStruct((n_tok * n_top // LANES, LANES), jnp.int32)),
        in_specs=[vmem] * 5 + [hbm] * 3,
        out_specs=(hbm, hbm, vmem, vmem),
        scratch_shapes=[
            pltpu.VMEM((ranks, n_top, rows), jnp.int32), pltpu.VMEM((width, hidden), jnp.bfloat16),
            pltpu.VMEM((width, hidden), jnp.bfloat16), pltpu.VMEM((width, hidden), jnp.bfloat16),
            pltpu.VMEM((n_tok, chunks, LANES), jnp.bfloat16), pitched, pltpu.VMEM((TILE, hidden), jnp.bfloat16),
            pltpu.VMEM((TILE, width), jnp.bfloat16), pitched, pltpu.VMEM((2, TILE, chunks, LANES), jnp.float32),
            pltpu.VMEM((chunks * (size + 1), LANES), jnp.float32),
            dma, dma((2,)), dma, dma] + [dma((SPREAD_CHUNKS,))] * 4 + [dma((2, SPREAD_CHUNKS))] * 2
        + [dma((3,)), dma((3,)), dma((3,))],
        compiler_params=pltpu.CompilerParams(collective_id=0, has_side_effects=True, vmem_limit_bytes=60 << 20),
        name="front",
    )(hidden_in, gain, head, sig, own_idx, sg, su, sd)


def combine_kernel(n_chunk, lag, part, hid_hbm, out_ref, mine, near, far_in, zin, hid, t4, m_sem, h_sem,
                   d_send, d_recv, y_send, y_recv, z_send, z_recv, t_send):
    z, e = lax.axis_index("tp"), lax.axis_index("ep")
    rows = out_ref.shape[0]
    chunks = part.shape[1]
    size = rows // n_chunk
    core = e % 2
    pair = e + 1 - 2 * core
    far = (e + 2) % 4
    far_pair = (pair + 2) % 4
    n_z = 4
    zn = z + 1 - 2 * (z % 2)

    barrier = pltpu.get_barrier_semaphore()
    for dev in ({"ep": pair}, {"ep": far}):
        pl.semaphore_signal(barrier, inc=1, device_id=dev, device_id_type=MESH)

    @pl.when(z > 0)
    def _():
        pl.semaphore_signal(barrier, inc=1, device_id={"tp": z - 1}, device_id_type=MESH)

    @pl.when(z < n_z - 1)
    def _():
        pl.semaphore_signal(barrier, inc=1, device_id={"tp": z + 1}, device_id_type=MESH)
    at_end = (z == 0) | (z == n_z - 1)

    @pl.when(at_end)
    def _():
        pl.semaphore_wait(barrier, 3)

    @pl.when(jnp.logical_not(at_end))
    def _():
        pl.semaphore_wait(barrier, 4)

    def at(j):
        return pl.ds(j * size, size)

    def d_copy(j, side):
        owner = far_pair if side == 0 else pair
        return pltpu.make_async_remote_copy(
            part.at[pl.ds(owner * rows + j * size, size)], near.at[side, at(j)],
            d_send.at[side, j], d_recv.at[side, j], device_id={"ep": pair}, device_id_type=MESH)

    def m_copy(j, side):
        owner = far if side == 0 else e
        return pltpu.make_async_copy(part.at[pl.ds(owner * rows + j * size, size)], mine.at[side, at(j)], m_sem.at[side, j])

    def y_copy(j):
        return pltpu.make_async_remote_copy(
            mine.at[0, at(j)], far_in.at[at(j)], y_send.at[j], y_recv.at[j], device_id={"ep": far}, device_id_type=MESH)

    def z_copy(j, slot, to):
        return pltpu.make_async_remote_copy(
            mine.at[1, at(j)], zin.at[slot, at(j)], z_send.at[j], z_recv.at[slot, j], device_id={"tp": to}, device_id_type=MESH)

    def t_copy(j, side, to, src):
        return pltpu.make_async_remote_copy(
            src, zin.at[1, at(j)], t_send.at[side, j], z_recv.at[1, j], device_id={"tp": to}, device_id_type=MESH)

    hid_copy = pltpu.make_async_copy(hid_hbm, hid, h_sem)

    def first(j, _):
        for side in range(2):
            d_copy(j, side).start()
            m_copy(j, side).start()
        return 0
    lax.fori_loop(0, n_chunk, first, 0)
    hid_copy.start()

    def f32(ref):
        return ref[...].astype(jnp.float32)

    def finish(j, src):
        def put(g, _):
            for u in range(8):
                i = g * 8 + u
                t4[pl.ds(i, chunks, stride=size + 1), :] = src[i].astype(jnp.float32)
            return 0
        lax.fori_loop(0, size // 8, put, 0)
        for k in range(chunks):
            cols = slice(k * LANES, (k + 1) * LANES)
            tot = t4[k * (size + 1):k * (size + 1) + size, :]
            out_ref[at(j), cols] = (hid[at(j), cols].astype(jnp.float32) + tot).astype(jnp.bfloat16)

    def step(i, _):
        @pl.when(i < n_chunk)
        def _():
            for side in range(2):
                d_copy(i, side).wait_recv()
                m_copy(i, side).wait()
            mine[0, at(i)] = (f32(mine.at[0, at(i)]) + f32(near.at[0, at(i)])).astype(jnp.bfloat16)
            y_copy(i).start()

        def stage(shift):
            j = i - shift * lag
            odd = j % 2
            spot = z + odd * (n_z - 1 - 2 * z)
            ahead = 1 - 2 * odd
            return j, spot, ahead, (j >= 0) & (j < n_chunk)

        @pl.when(i == 3 * lag)
        def _():
            hid_copy.wait()

        j, spot, ahead, live = stage(1)

        @pl.when(live)
        def _():
            y_copy(j).wait_recv()
            mine[1, at(j)] = (f32(mine.at[1, at(j)]) + f32(near.at[1, at(j)]) + f32(far_in.at[at(j)])).astype(jnp.bfloat16)

            @pl.when(spot == 0)
            def _():
                z_copy(j, 0, z + ahead).start()

            @pl.when(spot == 3)
            def _():
                z_copy(j, 0, z - ahead).start()

        j2, spot2, ahead2, live2 = stage(2)

        @pl.when(live2 & (spot2 == 2))
        def _():
            z_copy(j2, 0, zn).wait_recv()
            mine[1, at(j2)] = (f32(mine.at[1, at(j2)]) + f32(zin.at[0, at(j2)])).astype(jnp.bfloat16)
            z_copy(j2, 1, z - ahead2).start()

        j3, spot3, ahead3, live3 = stage(3)

        @pl.when(live3 & (spot3 == 1))
        def _():
            z_copy(j3, 0, zn).wait_recv()
            z_copy(j3, 1, zn).wait_recv()
            mine[1, at(j3)] = (f32(mine.at[1, at(j3)]) + f32(zin.at[0, at(j3)]) + f32(zin.at[1, at(j3)])).astype(jnp.bfloat16)
            t_copy(j3, 0, z - ahead3, mine.at[1, at(j3)]).start()
            t_copy(j3, 1, z + ahead3, mine.at[1, at(j3)]).start()
            finish(j3, mine.at[1, at(j3)])

        j4, spot4, ahead4, live4 = stage(4)

        @pl.when(live4 & (spot4 == 2))
        def _():
            z_copy(j4, 1, zn).wait_recv()
            t_copy(j4, 0, z + ahead4, zin.at[1, at(j4)]).start()
            finish(j4, zin.at[1, at(j4)])

        j5, spot5, ahead5, live5 = stage(5)

        @pl.when(live5 & ((spot5 == 0) | (spot5 == 3)))
        def _():
            z_copy(j5, 1, zn).wait_recv()
            finish(j5, zin.at[1, at(j5)])
        return 0
    lax.fori_loop(0, n_chunk + 5 * lag, step, 0)

    def drain(j, _):
        odd = j % 2
        spot = z + odd * (n_z - 1 - 2 * z)
        d_copy(j, 0).wait_send()
        d_copy(j, 1).wait_send()
        y_copy(j).wait_send()

        @pl.when(spot != 1)
        def _():
            z_copy(j, 0, zn).wait_send()

        @pl.when((spot == 1) | (spot == 2))
        def _():
            t_copy(j, 0, zn, mine.at[1, at(j)]).wait_send()

        @pl.when(spot == 1)
        def _():
            t_copy(j, 1, zn, mine.at[1, at(j)]).wait_send()
        return 0
    lax.fori_loop(0, n_chunk, drain, 0)


def combine(part, hidden_in, n_chunk, lag):
    rows, hidden = hidden_in.shape
    block = (rows,) + part.shape[1:]
    dma = pltpu.SemaphoreType.DMA
    size = rows // n_chunk
    hbm = pl.BlockSpec(memory_space=pl.ANY)
    return pl.pallas_call(
        functools.partial(combine_kernel, n_chunk, lag),
        out_shape=jax.ShapeDtypeStruct((rows, hidden), jnp.bfloat16),
        in_specs=[hbm, hbm],
        out_specs=pl.BlockSpec(memory_space=pltpu.VMEM),
        scratch_shapes=[
            pltpu.VMEM((2,) + block, jnp.bfloat16), pltpu.VMEM((2,) + block, jnp.bfloat16), pltpu.VMEM(block, jnp.bfloat16),
            pltpu.VMEM((2,) + block, jnp.bfloat16), pltpu.VMEM((rows, hidden), jnp.bfloat16),
            pltpu.VMEM(((size + 1) * part.shape[1] + 8, LANES), jnp.float32),
            dma((2, n_chunk)), dma, dma((2, n_chunk)), dma((2, n_chunk)), dma((n_chunk,)), dma((n_chunk,)),
            dma((n_chunk,)), dma((2, n_chunk)), dma((2, n_chunk)),
        ],
        compiler_params=pltpu.CompilerParams(collective_id=1, has_side_effects=True, vmem_limit_bytes=60 << 20),
        name="combine",
    )(part, hidden_in)


def solution(mesh):
    tok_spec = P(('dp', 'ep'), None)
    in_specs = (tok_spec, tok_spec, P(None), P(None, None), P(None, None),
                P('ep', None, 'tp'), P('ep', None, 'tp'), P('ep', 'tp', None),
                P(None, ('tp', 'ep')), P(None, ('tp', 'ep')), P(('tp', 'ep'), None))

    def local_step(hidden_in, topk_idx, norm_gain, router_w, shared_sig_w, exp_gate, exp_up, exp_down, sh_gate, sh_up, sh_down):
        all_h, sums, wt, all_idx = front(hidden_in, norm_gain[None, :], router_w.T, shared_sig_w.T, topk_idx.T,
                                         lax.axis_size('ep'), sh_gate.T, sh_up.T, sh_down)
        part = moe(all_idx, wt.reshape(-1), all_h, sums, jnp.swapaxes(exp_gate, 1, 2), jnp.swapaxes(exp_up, 1, 2), exp_down)
        return combine(part, hidden_in, COMBINE_CHUNKS, COMBINE_LAG)

    return jax.shard_map(local_step, mesh=mesh, in_specs=in_specs, out_specs=tok_spec, check_vma=False)
```

```python
import functools
import math

import jax
import jax.numpy as jnp
from jax import lax
from jax.experimental import pallas as pl
from jax.experimental.pallas import tpu as pltpu
from jax.sharding import PartitionSpec as P

RMS_EPS = 1e-6
LANES = 128
TILE = 256
PITCH = TILE + 1
GROUP = 8
TOK_MASK = 8191
MESH = pl.DeviceIdType.MESH
SPREAD_CHUNKS = 16
COMBINE_CHUNKS = 64
COMBINE_LAG = 3


def dot_t(a, b):
    return lax.dot_general(a, b, (((1,), (1,)), ((), ())), preferred_element_type=jnp.float32)


def routing(idx_ref, first, ranks, n_tok, n_local, n_row, pos_v, list_v, in_row, totals):
    n = idx_ref.shape[0]
    i32, bf16, f32 = jnp.int32, jnp.bfloat16, jnp.float32
    sub = lax.broadcasted_iota(i32, (LANES, LANES), 0)
    lane = lax.broadcasted_iota(i32, (LANES, LANES), 1)
    below = jnp.where(sub < lane, 1.0, 0.0).astype(bf16)
    above = jnp.where(lane < sub, 1.0, 0.0).astype(bf16)
    ones = jnp.ones((LANES, LANES), bf16)

    def mask(e):
        return jnp.where(idx_ref[...] == first + e, 1.0, 0.0)

    both = jnp.concatenate([below, ones], axis=1)
    for e in range(n_local):
        got = jnp.dot(mask(e).astype(bf16), both, preferred_element_type=f32)
        in_row[e * n:(e + 1) * n, :] = got[:, :LANES]
        totals[e * n:(e + 1) * n, :] = got[:, LANES:]
    pos = jnp.zeros((n, LANES), f32)
    start = jnp.zeros((1, LANES), i32)
    for e in range(n_local):
        total = totals[e * n:(e + 1) * n, :]
        before = jnp.dot(above, total.astype(bf16), preferred_element_type=f32)
        count = (before[n - 1:n] + total[n - 1:n]).astype(i32)
        tiles = (count + TILE - 1) // TILE
        list_v[n_row + e:n_row + e + 1, :] = tiles
        pos += mask(e) * (in_row[e * n:(e + 1) * n, :] + before + (start * TILE).astype(f32) + 1.0)
        start += tiles
    pos_v[...] = pos.astype(i32) - 1

    rows = lax.broadcasted_iota(i32, (n_row, LANES), 0)
    step = 8
    nb = n_tok // ranks // LANES
    n_top = n * LANES // n_tok
    base = n_tok // LANES
    lane_val = lax.broadcasted_iota(i32, (LANES, LANES), 1).astype(f32)

    def add(g, acc):
        lhs, rhs = [], []
        for u in range(step):
            r = g * step + u
            p = pos_v[pl.ds(r, 1), :]
            tok_row = r // (nb * n_top) * nb + r % nb
            code = (r // nb % n_top * ((TOK_MASK + 1) // LANES) + tok_row - base).astype(f32)
            lhs.append(jnp.where(rows == p // LANES, 1.0, 0.0).astype(bf16))
            hit = sub == jnp.where(p < 0, LANES, p % LANES)
            rhs.append(jnp.concatenate([jnp.where(hit, code, 0.0), jnp.where(hit, lane_val, 0.0)], axis=0).astype(bf16))
        return acc + dot_t(jnp.concatenate(lhs, axis=1), jnp.concatenate(rhs, axis=1))
    acc = lax.fori_loop(0, n // step, add, jnp.zeros((n_row, 2 * LANES), f32))
    list_v[0:n_row, :] = (acc[:, :LANES] * LANES + acc[:, LANES:]).astype(i32) + n_tok


def moe_kernel(idx_ref, wt_hbm, h_hbm, sum_hbm, eg, eu, ed, out_hbm,
               hv, acc, wg, wu, wd, x4, xb, act, y4, pos_v, list_v, list_ref, tile_exp, wt_ref, h_sem, s_sem, w_sem, o_sem, l_sem, t_sem):
    n_tok, chunks, _ = h_hbm.shape
    n_local, width, _ = ed.shape
    n_row = list_v.shape[0] - 16
    span = TILE // LANES
    last = n_row // span - 1

    def weight_starts(e, slot):
        def start(k, _):
            cols = pl.ds(pl.multiple_of(k * LANES, LANES), LANES)
            for i, (s, d) in enumerate(((eg, wg), (eu, wu), (ed, wd))):
                pltpu.make_async_copy(s.at[e, :, cols], d.at[slot, k], w_sem.at[slot, i]).start()
            return 0
        lax.fori_loop(0, chunks, start, 0)

    def weight_waits(slot):
        for i, d in enumerate((wg, wu, wd)):
            pltpu.make_async_copy(d.at[slot], d.at[slot], w_sem.at[slot, i]).wait()

    def columns(ref, lo, hi):
        return jnp.concatenate([ref[k] for k in range(lo, hi)], axis=1)

    h_copy = pltpu.make_async_copy(h_hbm, hv.at[pl.ds(0, n_tok)], h_sem)
    s_copy = pltpu.make_async_copy(sum_hbm, acc.at[pl.ds(0, n_tok)], s_sem)
    t_copy = pltpu.make_async_copy(wt_hbm, wt_ref, t_sem)
    h_copy.start()
    t_copy.start()
    s_copy.start()
    routing(idx_ref, lax.axis_index("ep") * n_local, lax.axis_size("ep"), n_tok, n_local, n_row, pos_v, list_v, x4, y4)
    l_copy = pltpu.make_async_copy(list_v, list_ref, l_sem)
    l_copy.start()
    l_copy.wait()

    def exp_tiles(e):
        return list_ref[n_row + e, 0]

    def fill(e, t):
        def put(j, _):
            tile_exp[t + j] = e
            return 0
        count = exp_tiles(e)
        lax.fori_loop(0, count, put, 0)
        return t + count
    n_tile = lax.fori_loop(0, n_local, fill, 0)

    @pl.when(n_tile > 0)
    def _():
        weight_starts(tile_exp[0], 0)
    h_copy.wait()
    t_copy.wait()

    def gather(base, g):
        for u in range(GROUP):
            i = g * GROUP + u
            tok = list_ref[base * span + i // LANES, i % LANES] & TOK_MASK
            x4[pl.ds(i, chunks, stride=PITCH), :] = hv[tok].astype(jnp.float32)

    def pack(k):
        xb[k] = x4[k * PITCH:k * PITCH + TILE, :].astype(jnp.bfloat16)

    def scatter(base, g):
        sums = []
        for u in range(GROUP):
            i = g * GROUP + u
            entry = list_ref[base * span + i // LANES, i % LANES]
            tok = entry & TOK_MASK
            sums.append((tok, acc[tok] + y4[pl.ds(i, chunks, stride=PITCH), :] * wt_ref[entry]))
        for tok, v in sums:
            acc[tok] = v

    def loop(fn, base):
        for g in range(TILE // GROUP):
            fn(base, g)

    loop(gather, 0)
    for k in range(chunks):
        pack(k)
    def tile(t, slot):
        e = tile_exp[t]
        fresh = (t == 0) | (e != tile_exp[jnp.maximum(t - 1, 0)])
        slot = jnp.where(fresh, 1 - slot, slot)

        @pl.when(fresh)
        def _():
            weight_waits(slot)
            after = t + exp_tiles(e)

            @pl.when(after < n_tile)
            def _():
                weight_starts(tile_exp[after], 1 - slot)

        @pl.when(t == 1)
        def _():
            s_copy.wait()

        prev = jnp.where(t == 0, last, t - 1)
        n_group = TILE // GROUP
        x = columns(xb, 0, chunks)
        gate = dot_t(x, columns(wg.at[slot], 0, chunks))
        up = dot_t(x, columns(wu.at[slot], 0, chunks))
        for g in range(n_group):
            scatter(prev, g)
        act[...] = (jax.nn.silu(gate) * up).astype(jnp.bfloat16)
        for g in range(n_group):
            gather(t + 1, g)
        for k in range(0, chunks, 2):
            d = jnp.dot(act[...], columns(wd.at[slot], k, k + 2), preferred_element_type=jnp.float32)
            y4[k * PITCH:k * PITCH + TILE, :] = d[:, :LANES]
            y4[(k + 1) * PITCH:(k + 1) * PITCH + TILE, :] = d[:, LANES:]
        for k in range(chunks):
            pack(k)
        return slot

    lax.fori_loop(0, n_tile, tile, 1)

    @pl.when(n_tile <= 1)
    def _():
        s_copy.wait()
    loop(scatter, jnp.where(n_tile == 0, last, n_tile - 1))

    blk = 256

    def flush(i, _):
        def conv(j, _):
            r = i * blk + j * 16
            hv[pl.ds(r, 16)] = acc[pl.ds(r, 16)].astype(jnp.bfloat16)
            return 0
        lax.fori_loop(0, blk // 16, conv, 0)
        pltpu.make_async_copy(hv.at[pl.ds(i * blk, blk)], out_hbm.at[pl.ds(i * blk, blk)], o_sem).start()
        return 0
    lax.fori_loop(0, n_tok // blk, flush, 0)
    pltpu.make_async_copy(hv.at[pl.ds(0, n_tok)], out_hbm, o_sem).wait()


def moe(idx, wt, h3, sums, eg, eu, ed):
    n_tok, chunks, _ = h3.shape
    hidden = chunks * LANES
    width = ed.shape[1]
    hbm = pl.BlockSpec(memory_space=pl.ANY)
    max_tiles = -(-(idx.size + eg.shape[0] * (TILE - 1)) // TILE) + 1
    n_row = -(-max_tiles * TILE // (16 * LANES)) * 16
    return pl.pallas_call(
        moe_kernel,
        out_shape=jax.ShapeDtypeStruct((n_tok, chunks, LANES), jnp.bfloat16),
        in_specs=[pl.BlockSpec(memory_space=pltpu.VMEM)] + [hbm] * 6,
        out_specs=hbm,
        scratch_shapes=[
            pltpu.VMEM((n_tok + GROUP, chunks, LANES), jnp.bfloat16),
            pltpu.VMEM((n_tok + GROUP, chunks, LANES), jnp.float32),
            pltpu.VMEM((2, chunks, width, LANES), jnp.bfloat16),
            pltpu.VMEM((2, chunks, width, LANES), jnp.bfloat16),
            pltpu.VMEM((2, chunks, width, LANES), jnp.bfloat16),
            pltpu.VMEM((chunks * PITCH + 8, LANES), jnp.float32),
            pltpu.VMEM((chunks, TILE, LANES), jnp.bfloat16),
            pltpu.VMEM((TILE, width), jnp.bfloat16),
            pltpu.VMEM((chunks * PITCH + 8, LANES), jnp.float32),
            pltpu.VMEM(idx.shape, jnp.int32),
            pltpu.VMEM((n_row + 16, LANES), jnp.int32),
            pltpu.SMEM((n_row + 16, LANES), jnp.int32),
            pltpu.SMEM((max_tiles + 1,), jnp.int32),
            pltpu.SMEM(wt.shape, jnp.float32),
            pltpu.SemaphoreType.DMA,
            pltpu.SemaphoreType.DMA,
            pltpu.SemaphoreType.DMA((2, 3)),
            pltpu.SemaphoreType.DMA,
            pltpu.SemaphoreType.DMA,
            pltpu.SemaphoreType.DMA,
        ],
        compiler_params=pltpu.CompilerParams(vmem_limit_bytes=67043328),
        cost_estimate=pl.CostEstimate(flops=2 * 3 * hidden * width * n_tok, bytes_accessed=130_000_000, transcendentals=0),
        name="moe",
    )(idx, wt, h3, sums, eg, eu, ed)


def front_kernel(hid, gain_ref, head_ref, sig_ref, own_idx, sg, su, sd, h_out, sum_out, wt_out, idx_out,
                 idx_ref, wg, wu, wd, hbuf, x4, xb, act, y4, stage, t4, h_sem, s_sem, pair_send, pair_recv, y_send, y_recv, z_send, z_recv,
                 fwd_send, fwd_recv, w_sem, i_send, i_recv):
    z, e = lax.axis_index("tp"), lax.axis_index("ep")
    rows, hidden = hid.shape
    chunks = hidden // LANES
    size = t4.shape[0] // chunks - 1
    n_chunk = rows // (2 * size)
    core = e % 2
    pair = e + 1 - 2 * core
    far = (e + 2) % 4
    far_pair = (pair + 2) % 4
    half = z % 2
    zpair = z + 1 - 2 * half

    barrier = pltpu.get_barrier_semaphore()
    for dev in ({"ep": pair}, {"ep": far}, {"ep": far_pair}, {"tp": zpair}):
        pl.semaphore_signal(barrier, inc=1, device_id=dev, device_id_type=MESH)
    w_copies = [pltpu.make_async_copy(s, d, w_sem.at[i])
                for i, (s, d) in enumerate(((sg, wg), (su, wu), (sd, wd)))]
    for c in w_copies:
        c.start()
    pl.semaphore_wait(barrier, 4)

    i_copies = [pltpu.make_async_remote_copy(
        own_idx, idx_ref.at[e], i_send.at[i], i_recv.at[i], device_id={"ep": dev}, device_id_type=MESH)
        for i, dev in enumerate((pair, far, far_pair))]
    for c in i_copies:
        c.start()
    idx_ref[e] = own_idx[...]

    def send_rows(block, h, j):
        return hbuf.at[pl.ds(block * rows + h * (rows // 2) + j * size, size)]

    def y_copy(j):
        mine = send_rows(e, half, j)
        return pltpu.make_async_remote_copy(mine, mine, y_send.at[j], y_recv.at[j], device_id={"ep": far}, device_id_type=MESH)

    def z_copy(j):
        got = send_rows(far, half, j)
        return pltpu.make_async_remote_copy(got, got, z_send.at[j], z_recv.at[j], device_id={"tp": zpair}, device_id_type=MESH)

    def fwd_copy(j, side):
        got = send_rows(far, half if side == 0 else 1 - half, j)
        return pltpu.make_async_remote_copy(
            got, got, fwd_send.at[side, j], fwd_recv.at[side, j], device_id={"ep": pair}, device_id_type=MESH)

    own = hbuf.at[pl.ds(e * rows, rows)]
    to_pair = pltpu.make_async_remote_copy(own, own, pair_send, pair_recv, device_id={"ep": pair}, device_id_type=MESH)
    gain = gain_ref[...].astype(jnp.float32).reshape(1, -1)

    def norm(c, _):
        lo = (half * n_chunk + c) % (2 * n_chunk) * size
        x = hid[pl.ds(lo, size), :].astype(jnp.float32)
        inv_rms = lax.rsqrt(jnp.mean(x * x, axis=-1, keepdims=True) + RMS_EPS)
        h = (x * inv_rms * gain).astype(jnp.bfloat16).astype(jnp.float32)
        for k in range(chunks):
            t4[k * (size + 1):k * (size + 1) + size, :] = h[:, k * LANES:(k + 1) * LANES]
        for i in range(size):
            hbuf[e * rows + lo + i] = t4[pl.ds(i, chunks, stride=size + 1), :].astype(jnp.bfloat16)

        @pl.when(c < n_chunk)
        def _():
            y_copy(c).start()
        return 0
    lax.fori_loop(0, 2 * n_chunk, norm, 0)
    to_pair.start()
    for c in w_copies:
        c.wait()

    def relay_y(j):
        y_copy(j).wait_recv()
        z_copy(j).start()
        fwd_copy(j, 0).start()

    def relay_z(j):
        z_copy(j).wait_recv()
        fwd_copy(j, 1).start()

    n_tile = 4 * rows // TILE
    per = rows // TILE
    quarter = n_chunk // 2
    half_step, flight = 1.7, 45.0 / n_chunk
    due = {}
    for j in range(n_chunk):
        y_at = 5 + flight * (j + 1)
        for kind, at_time, need in (("y", y_at, 16 if j < quarter else 24), ("z", y_at + flight + 3, 20 if j < quarter else 28)):
            q = min(need, max(0, math.ceil((at_time - 5) / half_step)))
            due.setdefault(q, []).append((at_time, kind, j))
    due.setdefault(8, []).append((0, "p", 0))
    for q, kind, j in ((18, "a", 0), (22, "b", 0), (26, "a", 1), (30, "b", 1)):
        due.setdefault(q, []).append((1e3, kind, j))

    def h_rows(base):
        return pltpu.make_async_copy(hbuf.at[pl.ds(base, TILE)], h_out.at[pl.ds(base, TILE)], h_sem)

    def do(what):
        _, kind, arg = what
        if kind == "p":
            to_pair.wait_recv()
            for c in i_copies:
                c.wait_recv()
            ranks, n_top, _ = idx_ref.shape
            nb = rows // LANES
            for r in range(ranks * n_top * nb):
                b = r % nb
                idx_out[r:r + 1, :] = idx_ref[r // (n_top * nb), r // nb % n_top:r // nb % n_top + 1, b * LANES:(b + 1) * LANES]
        elif kind == "y":
            relay_y(arg)
        elif kind == "z":
            relay_z(arg)
        else:
            for j in range(quarter):
                fwd_copy(arg * quarter + j, 0 if kind == "a" else 1).wait_recv()

    def sum_copy(base, slot):
        return pltpu.make_async_copy(stage.at[slot], sum_out.at[pl.ds(base, TILE)], s_sem.at[slot])

    sig = sig_ref[...].astype(jnp.float32)

    def relay(q, parity):
        for at_step, what in due.items():
            if at_step % 2 == parity:
                @pl.when(q == at_step)
                def _(what=what):
                    for w in sorted(what):
                        do(w)

    def tile(s, _):
        relay(2 * s, 0)
        u = s - 2 * per
        near = s // per
        near_block = e + near * (pair - e)
        near_base = near_block * rows + s % per * TILE
        far_block = far + u % 2 * (far_pair - far)
        far_half = half + u // 2 % 2 * (1 - 2 * half)
        far_base = far_block * rows + far_half * (rows // 2) + u // 4 * TILE
        is_far = s // (2 * per)
        base = pl.multiple_of(near_base + is_far * (far_base - near_base), TILE)
        block = near_block + is_far * (far_block - near_block)
        col = pl.multiple_of(base - block * rows, TILE)
        slot = s % 2

        def fill(g, _):
            for v in range(16):
                i = g * 16 + v
                x4[pl.ds(i, chunks, stride=PITCH), :] = hbuf[base + i].astype(jnp.float32)
            return 0
        lax.fori_loop(0, TILE // 16, fill, 0)
        for k in range(chunks):
            xb[:, k * LANES:(k + 1) * LANES] = x4[k * PITCH:k * PITCH + TILE, :].astype(jnp.bfloat16)

        logits = dot_t(head_ref[...], xb[...])
        prob = jnp.exp(logits - jnp.max(logits, axis=0, keepdims=True))
        prob = prob / jnp.sum(prob, axis=0, keepdims=True)
        expert = lax.broadcasted_iota(jnp.int32, prob.shape, 0)
        idx = idx_ref[block, :, pl.ds(col, TILE)]
        picked = [jnp.sum(jnp.where(expert == idx[k:k + 1, :], prob, 0.0), axis=0, keepdims=True) for k in range(idx.shape[0])]
        wt_out[:, pl.ds(base, TILE)] = jnp.concatenate(picked, axis=0)

        gate = dot_t(xb[...], wg[...])
        up = dot_t(xb[...], wu[...])
        act[...] = (jax.nn.silu(gate) * up).astype(jnp.bfloat16)
        scale = jax.nn.sigmoid(jnp.sum(xb[...].astype(jnp.float32) * sig, axis=1, keepdims=True))
        for k in range(0, chunks, 2):
            d = jnp.dot(act[...], wd[:, k * LANES:(k + 2) * LANES], preferred_element_type=jnp.float32) * scale
            y4[k * PITCH:k * PITCH + TILE, :] = d[:, :LANES]
            y4[(k + 1) * PITCH:(k + 1) * PITCH + TILE, :] = d[:, LANES:]

        relay(2 * s + 1, 1)
        h_rows(base).start()

        @pl.when(s >= 2)
        def _():
            sum_copy(0, slot).wait()

        def put(g, _):
            for v in range(16):
                i = g * 16 + v
                stage[slot, i] = y4[pl.ds(i, chunks, stride=PITCH), :]
            return 0
        lax.fori_loop(0, TILE // 16, put, 0)
        sum_copy(base, slot).start()
        return 0
    lax.fori_loop(0, n_tile, tile, 0)

    def drain(j, _):
        fwd_copy(j, 0).wait_send()
        fwd_copy(j, 1).wait_send()
        y_copy(j).wait_send()
        z_copy(j).wait_send()
        return 0
    lax.fori_loop(0, n_chunk, drain, 0)
    to_pair.wait_send()
    for c in i_copies:
        c.wait_send()
    pltpu.make_async_copy(hbuf, h_out, h_sem).wait()
    sum_copy(0, 0).wait()
    sum_copy(0, 1).wait()


def front(hidden_in, gain, head, sig, own_idx, ranks, sg, su, sd):
    rows, hidden = hidden_in.shape
    n_top = own_idx.shape[0]
    width = sg.shape[0]
    chunks = hidden // LANES
    n_tok = ranks * rows
    size = rows // (2 * SPREAD_CHUNKS)
    dma = pltpu.SemaphoreType.DMA
    vmem = pl.BlockSpec(memory_space=pltpu.VMEM)
    hbm = pl.BlockSpec(memory_space=pl.ANY)
    pitched = pltpu.VMEM((chunks * PITCH + 8, LANES), jnp.float32)
    return pl.pallas_call(
        front_kernel,
        out_shape=(jax.ShapeDtypeStruct((n_tok, chunks, LANES), jnp.bfloat16),
                   jax.ShapeDtypeStruct((n_tok, chunks, LANES), jnp.float32),
                   jax.ShapeDtypeStruct((n_top, TOK_MASK + 1), jnp.float32),
                   jax.ShapeDtypeStruct((n_tok * n_top // LANES, LANES), jnp.int32)),
        in_specs=[vmem] * 5 + [hbm] * 3,
        out_specs=(hbm, hbm, vmem, vmem),
        scratch_shapes=[
            pltpu.VMEM((ranks, n_top, rows), jnp.int32), pltpu.VMEM((width, hidden), jnp.bfloat16),
            pltpu.VMEM((width, hidden), jnp.bfloat16), pltpu.VMEM((width, hidden), jnp.bfloat16),
            pltpu.VMEM((n_tok, chunks, LANES), jnp.bfloat16), pitched, pltpu.VMEM((TILE, hidden), jnp.bfloat16),
            pltpu.VMEM((TILE, width), jnp.bfloat16), pitched, pltpu.VMEM((2, TILE, chunks, LANES), jnp.float32),
            pltpu.VMEM((chunks * (size + 1), LANES), jnp.float32),
            dma, dma((2,)), dma, dma] + [dma((SPREAD_CHUNKS,))] * 4 + [dma((2, SPREAD_CHUNKS))] * 2
        + [dma((3,)), dma((3,)), dma((3,))],
        compiler_params=pltpu.CompilerParams(collective_id=0, has_side_effects=True, vmem_limit_bytes=60 << 20),
        name="front",
    )(hidden_in, gain, head, sig, own_idx, sg, su, sd)


def combine_kernel(n_chunk, lag, part, hid, out_ref, mine, near, far_in, zin, t4, m_sem,
                   d_send, d_recv, y_send, y_recv, z_send, z_recv, t_send):
    z, e = lax.axis_index("tp"), lax.axis_index("ep")
    rows = out_ref.shape[0]
    chunks = part.shape[1]
    size = rows // n_chunk
    core = e % 2
    pair = e + 1 - 2 * core
    far = (e + 2) % 4
    far_pair = (pair + 2) % 4
    n_z = 4
    zn = z + 1 - 2 * (z % 2)

    barrier = pltpu.get_barrier_semaphore()
    for dev in ({"ep": pair}, {"ep": far}):
        pl.semaphore_signal(barrier, inc=1, device_id=dev, device_id_type=MESH)

    @pl.when(z > 0)
    def _():
        pl.semaphore_signal(barrier, inc=1, device_id={"tp": z - 1}, device_id_type=MESH)

    @pl.when(z < n_z - 1)
    def _():
        pl.semaphore_signal(barrier, inc=1, device_id={"tp": z + 1}, device_id_type=MESH)
    at_end = (z == 0) | (z == n_z - 1)

    @pl.when(at_end)
    def _():
        pl.semaphore_wait(barrier, 3)

    @pl.when(jnp.logical_not(at_end))
    def _():
        pl.semaphore_wait(barrier, 4)

    def at(j):
        return pl.ds(j * size, size)

    def d_copy(j, side):
        owner = far_pair if side == 0 else pair
        return pltpu.make_async_remote_copy(
            part.at[pl.ds(owner * rows + j * size, size)], near.at[side, at(j)],
            d_send.at[side, j], d_recv.at[side, j], device_id={"ep": pair}, device_id_type=MESH)

    def m_copy(j, side):
        owner = far if side == 0 else e
        return pltpu.make_async_copy(part.at[pl.ds(owner * rows + j * size, size)], mine.at[side, at(j)], m_sem.at[side, j])

    def y_copy(j):
        return pltpu.make_async_remote_copy(
            mine.at[0, at(j)], far_in.at[at(j)], y_send.at[j], y_recv.at[j], device_id={"ep": far}, device_id_type=MESH)

    def z_copy(j, slot, to):
        return pltpu.make_async_remote_copy(
            mine.at[1, at(j)], zin.at[slot, at(j)], z_send.at[j], z_recv.at[slot, j], device_id={"tp": to}, device_id_type=MESH)

    def t_copy(j, side, to, src):
        return pltpu.make_async_remote_copy(
            src, zin.at[1, at(j)], t_send.at[side, j], z_recv.at[1, j], device_id={"tp": to}, device_id_type=MESH)

    def first(j, _):
        for side in range(2):
            d_copy(j, side).start()
            m_copy(j, side).start()
        return 0
    lax.fori_loop(0, n_chunk, first, 0)

    def f32(ref):
        return ref[...].astype(jnp.float32)

    def finish(j, src):
        def put(g, _):
            for u in range(8):
                i = g * 8 + u
                t4[pl.ds(i, chunks, stride=size + 1), :] = src[i].astype(jnp.float32)
            return 0
        lax.fori_loop(0, size // 8, put, 0)
        for k in range(chunks):
            cols = slice(k * LANES, (k + 1) * LANES)
            tot = t4[k * (size + 1):k * (size + 1) + size, :]
            out_ref[at(j), cols] = (hid[at(j), cols].astype(jnp.float32) + tot).astype(jnp.bfloat16)

    def step(i, _):
        @pl.when(i < n_chunk)
        def _():
            for side in range(2):
                d_copy(i, side).wait_recv()
                m_copy(i, side).wait()
            mine[0, at(i)] = (f32(mine.at[0, at(i)]) + f32(near.at[0, at(i)])).astype(jnp.bfloat16)
            y_copy(i).start()

        def stage(shift):
            j = i - shift * lag
            odd = j % 2
            spot = z + odd * (n_z - 1 - 2 * z)
            ahead = 1 - 2 * odd
            return j, spot, ahead, (j >= 0) & (j < n_chunk)

        j, spot, ahead, live = stage(1)

        @pl.when(live)
        def _():
            y_copy(j).wait_recv()
            mine[1, at(j)] = (f32(mine.at[1, at(j)]) + f32(near.at[1, at(j)]) + f32(far_in.at[at(j)])).astype(jnp.bfloat16)

            @pl.when(spot == 0)
            def _():
                z_copy(j, 0, z + ahead).start()

            @pl.when(spot == 3)
            def _():
                z_copy(j, 0, z - ahead).start()

        j2, spot2, ahead2, live2 = stage(2)

        @pl.when(live2 & (spot2 == 2))
        def _():
            z_copy(j2, 0, zn).wait_recv()
            mine[1, at(j2)] = (f32(mine.at[1, at(j2)]) + f32(zin.at[0, at(j2)])).astype(jnp.bfloat16)
            z_copy(j2, 1, z - ahead2).start()

        j3, spot3, ahead3, live3 = stage(3)

        @pl.when(live3 & (spot3 == 1))
        def _():
            z_copy(j3, 0, zn).wait_recv()
            z_copy(j3, 1, zn).wait_recv()
            mine[1, at(j3)] = (f32(mine.at[1, at(j3)]) + f32(zin.at[0, at(j3)]) + f32(zin.at[1, at(j3)])).astype(jnp.bfloat16)
            t_copy(j3, 0, z - ahead3, mine.at[1, at(j3)]).start()
            t_copy(j3, 1, z + ahead3, mine.at[1, at(j3)]).start()
            finish(j3, mine.at[1, at(j3)])

        j4, spot4, ahead4, live4 = stage(4)

        @pl.when(live4 & (spot4 == 2))
        def _():
            z_copy(j4, 1, zn).wait_recv()
            t_copy(j4, 0, z + ahead4, zin.at[1, at(j4)]).start()
            finish(j4, zin.at[1, at(j4)])

        j5, spot5, ahead5, live5 = stage(5)

        @pl.when(live5 & ((spot5 == 0) | (spot5 == 3)))
        def _():
            z_copy(j5, 1, zn).wait_recv()
            finish(j5, zin.at[1, at(j5)])
        return 0
    lax.fori_loop(0, n_chunk + 5 * lag, step, 0)

    def drain(j, _):
        odd = j % 2
        spot = z + odd * (n_z - 1 - 2 * z)
        d_copy(j, 0).wait_send()
        d_copy(j, 1).wait_send()
        y_copy(j).wait_send()

        @pl.when(spot != 1)
        def _():
            z_copy(j, 0, zn).wait_send()

        @pl.when((spot == 1) | (spot == 2))
        def _():
            t_copy(j, 0, zn, mine.at[1, at(j)]).wait_send()

        @pl.when(spot == 1)
        def _():
            t_copy(j, 1, zn, mine.at[1, at(j)]).wait_send()
        return 0
    lax.fori_loop(0, n_chunk, drain, 0)


def combine(part, hidden_in, n_chunk, lag):
    rows, hidden = hidden_in.shape
    block = (rows,) + part.shape[1:]
    dma = pltpu.SemaphoreType.DMA
    size = rows // n_chunk
    hbm = pl.BlockSpec(memory_space=pl.ANY)
    return pl.pallas_call(
        functools.partial(combine_kernel, n_chunk, lag),
        out_shape=jax.ShapeDtypeStruct((rows, hidden), jnp.bfloat16),
        in_specs=[hbm, pl.BlockSpec(memory_space=pltpu.VMEM)],
        out_specs=pl.BlockSpec(memory_space=pltpu.VMEM),
        scratch_shapes=[
            pltpu.VMEM((2,) + block, jnp.bfloat16), pltpu.VMEM((2,) + block, jnp.bfloat16), pltpu.VMEM(block, jnp.bfloat16),
            pltpu.VMEM((2,) + block, jnp.bfloat16),
            pltpu.VMEM(((size + 1) * part.shape[1] + 8, LANES), jnp.float32),
            dma((2, n_chunk)), dma((2, n_chunk)), dma((2, n_chunk)), dma((n_chunk,)), dma((n_chunk,)),
            dma((n_chunk,)), dma((2, n_chunk)), dma((2, n_chunk)),
        ],
        compiler_params=pltpu.CompilerParams(collective_id=1, has_side_effects=True, vmem_limit_bytes=40 << 20),
        name="combine",
    )(part, hidden_in)


def solution(mesh):
    tok_spec = P(('dp', 'ep'), None)
    in_specs = (tok_spec, tok_spec, P(None), P(None, None), P(None, None),
                P('ep', None, 'tp'), P('ep', None, 'tp'), P('ep', 'tp', None),
                P(None, ('tp', 'ep')), P(None, ('tp', 'ep')), P(('tp', 'ep'), None))

    def local_step(hidden_in, topk_idx, norm_gain, router_w, shared_sig_w, exp_gate, exp_up, exp_down, sh_gate, sh_up, sh_down):
        all_h, sums, wt, all_idx = front(hidden_in, norm_gain, router_w.T, shared_sig_w.T, topk_idx.T,
                                         lax.axis_size('ep'), sh_gate.T, sh_up.T, sh_down)
        part = moe(all_idx, wt.reshape(-1), all_h, sums, jnp.swapaxes(exp_gate, 1, 2), jnp.swapaxes(exp_up, 1, 2), exp_down)
        return combine(part, hidden_in, COMBINE_CHUNKS, COMBINE_LAG)

    return jax.shard_map(local_step, mesh=mesh, in_specs=in_specs, out_specs=tok_spec, check_vma=False)
```

```python
import functools
import math

import jax
import jax.numpy as jnp
from jax import lax
from jax.experimental import pallas as pl
from jax.experimental.pallas import tpu as pltpu
from jax.sharding import PartitionSpec as P

RMS_EPS = 1e-6
LANES = 128
TILE = 256
PITCH = TILE + 1
GROUP = 8
TOK_MASK = 8191
MESH = pl.DeviceIdType.MESH
SPREAD_CHUNKS = 16
COMBINE_CHUNKS = 64
COMBINE_LAG = 3


def dot_t(a, b):
    return lax.dot_general(a, b, (((1,), (1,)), ((), ())), preferred_element_type=jnp.float32)


def columns(ref, lo, hi):
    return jnp.concatenate([ref[k] for k in range(lo, hi)], axis=1)


def routing(idx_ref, first, ranks, n_tok, n_local, n_row, pos_v, list_v, in_row, totals):
    n = idx_ref.shape[0]
    i32, bf16, f32 = jnp.int32, jnp.bfloat16, jnp.float32
    sub = lax.broadcasted_iota(i32, (LANES, LANES), 0)
    lane = lax.broadcasted_iota(i32, (LANES, LANES), 1)
    below = jnp.where(sub < lane, 1.0, 0.0).astype(bf16)
    above = jnp.where(lane < sub, 1.0, 0.0).astype(bf16)
    ones = jnp.ones((LANES, LANES), bf16)

    def mask(e):
        return jnp.where(idx_ref[...] == first + e, 1.0, 0.0)

    both = jnp.concatenate([below, ones], axis=1)
    for e in range(n_local):
        got = jnp.dot(mask(e).astype(bf16), both, preferred_element_type=f32)
        in_row[e * n:(e + 1) * n, :] = got[:, :LANES]
        totals[e * n:(e + 1) * n, :] = got[:, LANES:]
    pos = jnp.zeros((n, LANES), f32)
    start = jnp.zeros((1, LANES), i32)
    for e in range(n_local):
        total = totals[e * n:(e + 1) * n, :]
        before = jnp.dot(above, total.astype(bf16), preferred_element_type=f32)
        count = (before[n - 1:n] + total[n - 1:n]).astype(i32)
        tiles = (count + TILE - 1) // TILE
        list_v[n_row + e:n_row + e + 1, :] = tiles
        pos += mask(e) * (in_row[e * n:(e + 1) * n, :] + before + (start * TILE).astype(f32) + 1.0)
        start += tiles
    pos_v[...] = pos.astype(i32) - 1

    rows = lax.broadcasted_iota(i32, (n_row, LANES), 0)
    step = 8
    nb = n_tok // ranks // LANES
    n_top = n * LANES // n_tok
    base = n_tok // LANES
    lane_val = lax.broadcasted_iota(i32, (LANES, LANES), 1).astype(f32)

    def add(g, acc):
        lhs, rhs = [], []
        for u in range(step):
            r = g * step + u
            p = pos_v[pl.ds(r, 1), :]
            tok_row = r // (nb * n_top) * nb + r % nb
            code = (r // nb % n_top * ((TOK_MASK + 1) // LANES) + tok_row - base).astype(f32)
            lhs.append(jnp.where(rows == p // LANES, 1.0, 0.0).astype(bf16))
            hit = sub == jnp.where(p < 0, LANES, p % LANES)
            rhs.append(jnp.concatenate([jnp.where(hit, code, 0.0), jnp.where(hit, lane_val, 0.0)], axis=0).astype(bf16))
        return acc + dot_t(jnp.concatenate(lhs, axis=1), jnp.concatenate(rhs, axis=1))
    acc = lax.fori_loop(0, n // step, add, jnp.zeros((n_row, 2 * LANES), f32))
    list_v[0:n_row, :] = (acc[:, :LANES] * LANES + acc[:, LANES:]).astype(i32) + n_tok


def moe_kernel(idx_ref, wt_hbm, h_hbm, sum_hbm, eg, eu, ed, out_hbm,
               hv, acc, wg, wu, wd, x4, xb, act, y4, pos_v, list_v, list_ref, tile_exp, wt_ref, h_sem, s_sem, w_sem, o_sem, l_sem, t_sem):
    n_tok, chunks, _ = h_hbm.shape
    n_local, width, _ = ed.shape
    n_row = list_v.shape[0] - 16
    span = TILE // LANES
    last = n_row // span - 1

    def weight_starts(e, slot):
        def start(k, _):
            cols = pl.ds(pl.multiple_of(k * LANES, LANES), LANES)
            for i, (s, d) in enumerate(((eg, wg), (eu, wu), (ed, wd))):
                pltpu.make_async_copy(s.at[e, :, cols], d.at[slot, k], w_sem.at[slot, i]).start()
            return 0
        lax.fori_loop(0, chunks, start, 0)

    def weight_waits(slot):
        for i, d in enumerate((wg, wu, wd)):
            pltpu.make_async_copy(d.at[slot], d.at[slot], w_sem.at[slot, i]).wait()


    h_copy = pltpu.make_async_copy(h_hbm, hv.at[pl.ds(0, n_tok)], h_sem)
    s_copy = pltpu.make_async_copy(sum_hbm, acc.at[pl.ds(0, n_tok)], s_sem)
    t_copy = pltpu.make_async_copy(wt_hbm, wt_ref, t_sem)
    h_copy.start()
    t_copy.start()
    s_copy.start()
    routing(idx_ref, lax.axis_index("ep") * n_local, lax.axis_size("ep"), n_tok, n_local, n_row, pos_v, list_v, x4, y4)
    l_copy = pltpu.make_async_copy(list_v, list_ref, l_sem)
    l_copy.start()
    l_copy.wait()

    def exp_tiles(e):
        return list_ref[n_row + e, 0]

    def fill(e, t):
        def put(j, _):
            tile_exp[t + j] = e
            return 0
        count = exp_tiles(e)
        lax.fori_loop(0, count, put, 0)
        return t + count
    n_tile = lax.fori_loop(0, n_local, fill, 0)

    @pl.when(n_tile > 0)
    def _():
        weight_starts(tile_exp[0], 0)
    h_copy.wait()
    t_copy.wait()

    def gather(base, g):
        for u in range(GROUP):
            i = g * GROUP + u
            tok = list_ref[base * span + i // LANES, i % LANES] & TOK_MASK
            x4[pl.ds(i, chunks, stride=PITCH), :] = hv[tok].astype(jnp.float32)

    def pack(k):
        xb[k] = x4[k * PITCH:k * PITCH + TILE, :].astype(jnp.bfloat16)

    def scatter(base, g):
        sums = []
        for u in range(GROUP):
            i = g * GROUP + u
            entry = list_ref[base * span + i // LANES, i % LANES]
            tok = entry & TOK_MASK
            sums.append((tok, acc[tok] + y4[pl.ds(i, chunks, stride=PITCH), :] * wt_ref[entry]))
        for tok, v in sums:
            acc[tok] = v

    def loop(fn, base):
        for g in range(TILE // GROUP):
            fn(base, g)

    loop(gather, 0)
    for k in range(chunks):
        pack(k)
    def tile(t, slot):
        e = tile_exp[t]
        fresh = (t == 0) | (e != tile_exp[jnp.maximum(t - 1, 0)])
        slot = jnp.where(fresh, 1 - slot, slot)

        @pl.when(fresh)
        def _():
            weight_waits(slot)
            after = t + exp_tiles(e)

            @pl.when(after < n_tile)
            def _():
                weight_starts(tile_exp[after], 1 - slot)

        @pl.when(t == 1)
        def _():
            s_copy.wait()

        prev = jnp.where(t == 0, last, t - 1)
        n_group = TILE // GROUP
        x = columns(xb, 0, chunks)
        gate = dot_t(x, columns(wg.at[slot], 0, chunks))
        up = dot_t(x, columns(wu.at[slot], 0, chunks))
        for g in range(n_group):
            scatter(prev, g)
        act[...] = (jax.nn.silu(gate) * up).astype(jnp.bfloat16)
        for g in range(n_group):
            gather(t + 1, g)
        for k in range(0, chunks, 2):
            d = jnp.dot(act[...], columns(wd.at[slot], k, k + 2), preferred_element_type=jnp.float32)
            y4[k * PITCH:k * PITCH + TILE, :] = d[:, :LANES]
            y4[(k + 1) * PITCH:(k + 1) * PITCH + TILE, :] = d[:, LANES:]
        for k in range(chunks):
            pack(k)
        return slot

    lax.fori_loop(0, n_tile, tile, 1)

    @pl.when(n_tile <= 1)
    def _():
        s_copy.wait()
    loop(scatter, jnp.where(n_tile == 0, last, n_tile - 1))

    blk = 256

    def flush(i, _):
        def conv(j, _):
            r = i * blk + j * 16
            hv[pl.ds(r, 16)] = acc[pl.ds(r, 16)].astype(jnp.bfloat16)
            return 0
        lax.fori_loop(0, blk // 16, conv, 0)
        pltpu.make_async_copy(hv.at[pl.ds(i * blk, blk)], out_hbm.at[pl.ds(i * blk, blk)], o_sem).start()
        return 0
    lax.fori_loop(0, n_tok // blk, flush, 0)
    pltpu.make_async_copy(hv.at[pl.ds(0, n_tok)], out_hbm, o_sem).wait()


def moe(idx, wt, h3, sums, eg, eu, ed):
    n_tok, chunks, _ = h3.shape
    hidden = chunks * LANES
    width = ed.shape[1]
    hbm = pl.BlockSpec(memory_space=pl.ANY)
    max_tiles = -(-(idx.size + eg.shape[0] * (TILE - 1)) // TILE) + 1
    n_row = -(-max_tiles * TILE // (16 * LANES)) * 16
    return pl.pallas_call(
        moe_kernel,
        out_shape=jax.ShapeDtypeStruct((n_tok, chunks, LANES), jnp.bfloat16),
        in_specs=[pl.BlockSpec(memory_space=pltpu.VMEM)] + [hbm] * 6,
        out_specs=hbm,
        scratch_shapes=[
            pltpu.VMEM((n_tok + GROUP, chunks, LANES), jnp.bfloat16),
            pltpu.VMEM((n_tok + GROUP, chunks, LANES), jnp.float32),
            pltpu.VMEM((2, chunks, width, LANES), jnp.bfloat16),
            pltpu.VMEM((2, chunks, width, LANES), jnp.bfloat16),
            pltpu.VMEM((2, chunks, width, LANES), jnp.bfloat16),
            pltpu.VMEM((chunks * PITCH + 8, LANES), jnp.float32),
            pltpu.VMEM((chunks, TILE, LANES), jnp.bfloat16),
            pltpu.VMEM((TILE, width), jnp.bfloat16),
            pltpu.VMEM((chunks * PITCH + 8, LANES), jnp.float32),
            pltpu.VMEM(idx.shape, jnp.int32),
            pltpu.VMEM((n_row + 16, LANES), jnp.int32),
            pltpu.SMEM((n_row + 16, LANES), jnp.int32),
            pltpu.SMEM((max_tiles + 1,), jnp.int32),
            pltpu.SMEM(wt.shape, jnp.float32),
            pltpu.SemaphoreType.DMA,
            pltpu.SemaphoreType.DMA,
            pltpu.SemaphoreType.DMA((2, 3)),
            pltpu.SemaphoreType.DMA,
            pltpu.SemaphoreType.DMA,
            pltpu.SemaphoreType.DMA,
        ],
        compiler_params=pltpu.CompilerParams(vmem_limit_bytes=67043328),
        cost_estimate=pl.CostEstimate(flops=2 * 3 * hidden * width * n_tok, bytes_accessed=130_000_000, transcendentals=0),
        name="moe",
    )(idx, wt, h3, sums, eg, eu, ed)


def front_kernel(hid, gain_ref, head_ref, sig_ref, own_idx, sg, su, sd, h_out, sum_out, wt_out, idx_out,
                 idx_ref, wg, wu, wd, hbuf, x4, xb, act, y4, stage, t4, h_sem, s_sem, pair_send, pair_recv, y_send, y_recv, z_send, z_recv,
                 fwd_send, fwd_recv, w_sem, i_send, i_recv):
    z, e = lax.axis_index("tp"), lax.axis_index("ep")
    rows, hidden = hid.shape
    chunks = hidden // LANES
    size = t4.shape[0] // chunks - 1
    n_chunk = rows // (2 * size)
    core = e % 2
    pair = e + 1 - 2 * core
    far = (e + 2) % 4
    far_pair = (pair + 2) % 4
    half = z % 2
    zpair = z + 1 - 2 * half

    barrier = pltpu.get_barrier_semaphore()
    for dev in ({"ep": pair}, {"ep": far}, {"ep": far_pair}, {"tp": zpair}):
        pl.semaphore_signal(barrier, inc=1, device_id=dev, device_id_type=MESH)

    def load_weights(k, _):
        cols = pl.ds(pl.multiple_of(k * LANES, LANES), LANES)
        for i, (s, d) in enumerate(((sg, wg), (su, wu), (sd, wd))):
            pltpu.make_async_copy(s.at[:, cols], d.at[k], w_sem.at[i]).start()
        return 0
    lax.fori_loop(0, chunks, load_weights, 0)
    pl.semaphore_wait(barrier, 4)

    i_copies = [pltpu.make_async_remote_copy(
        own_idx, idx_ref.at[e], i_send.at[i], i_recv.at[i], device_id={"ep": dev}, device_id_type=MESH)
        for i, dev in enumerate((pair, far, far_pair))]
    for c in i_copies:
        c.start()
    idx_ref[e] = own_idx[...]

    def send_rows(block, h, j):
        return hbuf.at[pl.ds(block * rows + h * (rows // 2) + j * size, size)]

    def y_copy(j):
        mine = send_rows(e, half, j)
        return pltpu.make_async_remote_copy(mine, mine, y_send.at[j], y_recv.at[j], device_id={"ep": far}, device_id_type=MESH)

    def z_copy(j):
        got = send_rows(far, half, j)
        return pltpu.make_async_remote_copy(got, got, z_send.at[j], z_recv.at[j], device_id={"tp": zpair}, device_id_type=MESH)

    def fwd_copy(j, side):
        got = send_rows(far, half if side == 0 else 1 - half, j)
        return pltpu.make_async_remote_copy(
            got, got, fwd_send.at[side, j], fwd_recv.at[side, j], device_id={"ep": pair}, device_id_type=MESH)

    own = hbuf.at[pl.ds(e * rows, rows)]
    to_pair = pltpu.make_async_remote_copy(own, own, pair_send, pair_recv, device_id={"ep": pair}, device_id_type=MESH)
    gain = gain_ref[...].astype(jnp.float32).reshape(1, -1)

    def norm(c, _):
        lo = (half * n_chunk + c) % (2 * n_chunk) * size
        x = hid[pl.ds(lo, size), :].astype(jnp.float32)
        inv_rms = lax.rsqrt(jnp.mean(x * x, axis=-1, keepdims=True) + RMS_EPS)
        h = (x * inv_rms * gain).astype(jnp.bfloat16).astype(jnp.float32)
        for k in range(chunks):
            t4[k * (size + 1):k * (size + 1) + size, :] = h[:, k * LANES:(k + 1) * LANES]
        for i in range(size):
            hbuf[e * rows + lo + i] = t4[pl.ds(i, chunks, stride=size + 1), :].astype(jnp.bfloat16)

        @pl.when(c < n_chunk)
        def _():
            y_copy(c).start()
        return 0
    lax.fori_loop(0, 2 * n_chunk, norm, 0)
    to_pair.start()
    for i, d in enumerate((wg, wu, wd)):
        pltpu.make_async_copy(d, d, w_sem.at[i]).wait()

    def relay_y(j):
        y_copy(j).wait_recv()
        z_copy(j).start()
        fwd_copy(j, 0).start()

    def relay_z(j):
        z_copy(j).wait_recv()
        fwd_copy(j, 1).start()

    n_tile = 4 * rows // TILE
    per = rows // TILE
    quarter = n_chunk // 2
    half_step, flight = 1.9, 45.0 / n_chunk
    due = {}
    for j in range(n_chunk):
        y_at = 5 + flight * (j + 1)
        for kind, at_time, need in (("y", y_at, 16 if j < quarter else 24), ("z", y_at + flight + 3, 20 if j < quarter else 28)):
            q = min(need, max(0, math.ceil((at_time - 5) / half_step)))
            due.setdefault(q, []).append((at_time, kind, j))
    due.setdefault(8, []).append((0, "p", 0))
    for q, kind, j in ((18, "a", 0), (22, "b", 0), (26, "a", 1), (30, "b", 1)):
        due.setdefault(q, []).append((1e3, kind, j))

    def h_rows(base):
        return pltpu.make_async_copy(hbuf.at[pl.ds(base, TILE)], h_out.at[pl.ds(base, TILE)], h_sem)

    def do(what):
        _, kind, arg = what
        if kind == "p":
            to_pair.wait_recv()
            for c in i_copies:
                c.wait_recv()
            ranks, n_top, _ = idx_ref.shape
            nb = rows // LANES
            for r in range(ranks * n_top * nb):
                b = r % nb
                idx_out[r:r + 1, :] = idx_ref[r // (n_top * nb), r // nb % n_top:r // nb % n_top + 1, b * LANES:(b + 1) * LANES]
        elif kind == "y":
            relay_y(arg)
        elif kind == "z":
            relay_z(arg)
        else:
            for j in range(quarter):
                fwd_copy(arg * quarter + j, 0 if kind == "a" else 1).wait_recv()

    def sum_copy(base, slot):
        return pltpu.make_async_copy(stage.at[slot], sum_out.at[pl.ds(base, TILE)], s_sem.at[slot])

    sig = sig_ref[...].astype(jnp.float32)

    def relay(q, parity):
        for at_step, what in due.items():
            if at_step % 2 == parity:
                @pl.when(q == at_step)
                def _(what=what):
                    for w in sorted(what):
                        do(w)

    def tile(s, _):
        relay(2 * s, 0)
        u = s - 2 * per
        near = s // per
        near_block = e + near * (pair - e)
        near_base = near_block * rows + s % per * TILE
        far_block = far + u % 2 * (far_pair - far)
        far_half = half + u // 2 % 2 * (1 - 2 * half)
        far_base = far_block * rows + far_half * (rows // 2) + u // 4 * TILE
        is_far = s // (2 * per)
        base = pl.multiple_of(near_base + is_far * (far_base - near_base), TILE)
        block = near_block + is_far * (far_block - near_block)
        col = pl.multiple_of(base - block * rows, TILE)
        slot = s % 2

        def fill(g, _):
            for v in range(16):
                i = g * 16 + v
                x4[pl.ds(i, chunks, stride=PITCH), :] = hbuf[base + i].astype(jnp.float32)
            return 0
        lax.fori_loop(0, TILE // 16, fill, 0)
        for k in range(chunks):
            xb[k] = x4[k * PITCH:k * PITCH + TILE, :].astype(jnp.bfloat16)

        x = columns(xb, 0, chunks)
        logits = dot_t(head_ref[...], x)
        prob = jnp.exp(logits - jnp.max(logits, axis=0, keepdims=True))
        prob = prob / jnp.sum(prob, axis=0, keepdims=True)
        expert = lax.broadcasted_iota(jnp.int32, prob.shape, 0)
        idx = idx_ref[block, :, pl.ds(col, TILE)]
        picked = [jnp.sum(jnp.where(expert == idx[k:k + 1, :], prob, 0.0), axis=0, keepdims=True) for k in range(idx.shape[0])]
        for k, row in enumerate(picked):
            for b in range(TILE // LANES):
                wt_out[pl.ds(k * ((TOK_MASK + 1) // LANES) + base // LANES + b, 1), :] = row[:, b * LANES:(b + 1) * LANES]

        gate = dot_t(x, columns(wg, 0, chunks))
        up = dot_t(x, columns(wu, 0, chunks))
        act[...] = (jax.nn.silu(gate) * up).astype(jnp.bfloat16)
        scale = jax.nn.sigmoid(jnp.sum(x.astype(jnp.float32) * sig, axis=1, keepdims=True))
        for k in range(0, chunks, 2):
            d = jnp.dot(act[...], columns(wd, k, k + 2), preferred_element_type=jnp.float32) * scale
            y4[k * PITCH:k * PITCH + TILE, :] = d[:, :LANES]
            y4[(k + 1) * PITCH:(k + 1) * PITCH + TILE, :] = d[:, LANES:]

        relay(2 * s + 1, 1)
        h_rows(base).start()

        @pl.when(s >= 2)
        def _():
            sum_copy(0, slot).wait()

        def put(g, _):
            for v in range(16):
                i = g * 16 + v
                stage[slot, i] = y4[pl.ds(i, chunks, stride=PITCH), :]
            return 0
        lax.fori_loop(0, TILE // 16, put, 0)
        sum_copy(base, slot).start()
        return 0
    lax.fori_loop(0, n_tile, tile, 0)

    def drain(j, _):
        fwd_copy(j, 0).wait_send()
        fwd_copy(j, 1).wait_send()
        y_copy(j).wait_send()
        z_copy(j).wait_send()
        return 0
    lax.fori_loop(0, n_chunk, drain, 0)
    to_pair.wait_send()
    for c in i_copies:
        c.wait_send()
    pltpu.make_async_copy(hbuf, h_out, h_sem).wait()
    sum_copy(0, 0).wait()
    sum_copy(0, 1).wait()


def front(hidden_in, gain, head, sig, own_idx, ranks, sg, su, sd):
    rows, hidden = hidden_in.shape
    n_top = own_idx.shape[0]
    width = sg.shape[0]
    chunks = hidden // LANES
    n_tok = ranks * rows
    size = rows // (2 * SPREAD_CHUNKS)
    dma = pltpu.SemaphoreType.DMA
    vmem = pl.BlockSpec(memory_space=pltpu.VMEM)
    hbm = pl.BlockSpec(memory_space=pl.ANY)
    pitched = pltpu.VMEM((chunks * PITCH + 8, LANES), jnp.float32)
    return pl.pallas_call(
        front_kernel,
        out_shape=(jax.ShapeDtypeStruct((n_tok, chunks, LANES), jnp.bfloat16),
                   jax.ShapeDtypeStruct((n_tok, chunks, LANES), jnp.float32),
                   jax.ShapeDtypeStruct((n_top * (TOK_MASK + 1) // LANES, LANES), jnp.float32),
                   jax.ShapeDtypeStruct((n_tok * n_top // LANES, LANES), jnp.int32)),
        in_specs=[vmem] * 5 + [hbm] * 3,
        out_specs=(hbm, hbm, vmem, vmem),
        scratch_shapes=[
            pltpu.VMEM((ranks, n_top, rows), jnp.int32), pltpu.VMEM((chunks, width, LANES), jnp.bfloat16),
            pltpu.VMEM((chunks, width, LANES), jnp.bfloat16), pltpu.VMEM((chunks, width, LANES), jnp.bfloat16),
            pltpu.VMEM((n_tok, chunks, LANES), jnp.bfloat16), pitched, pltpu.VMEM((chunks, TILE, LANES), jnp.bfloat16),
            pltpu.VMEM((TILE, width), jnp.bfloat16), pitched, pltpu.VMEM((2, TILE, chunks, LANES), jnp.float32),
            pltpu.VMEM((chunks * (size + 1), LANES), jnp.float32),
            dma, dma((2,)), dma, dma] + [dma((SPREAD_CHUNKS,))] * 4 + [dma((2, SPREAD_CHUNKS))] * 2
        + [dma((3,)), dma((3,)), dma((3,))],
        compiler_params=pltpu.CompilerParams(collective_id=0, has_side_effects=True, vmem_limit_bytes=60 << 20),
        name="front",
    )(hidden_in, gain, head, sig, own_idx, sg, su, sd)


def combine_kernel(n_chunk, lag, part, hid, out_ref, mine, near, far_in, zin, t4, m_sem,
                   d_send, d_recv, y_send, y_recv, z_send, z_recv, t_send):
    z, e = lax.axis_index("tp"), lax.axis_index("ep")
    rows = out_ref.shape[0]
    chunks = part.shape[1]
    size = rows // n_chunk
    core = e % 2
    pair = e + 1 - 2 * core
    far = (e + 2) % 4
    far_pair = (pair + 2) % 4
    n_z = 4
    zn = z + 1 - 2 * (z % 2)

    barrier = pltpu.get_barrier_semaphore()
    for dev in ({"ep": pair}, {"ep": far}):
        pl.semaphore_signal(barrier, inc=1, device_id=dev, device_id_type=MESH)

    @pl.when(z > 0)
    def _():
        pl.semaphore_signal(barrier, inc=1, device_id={"tp": z - 1}, device_id_type=MESH)

    @pl.when(z < n_z - 1)
    def _():
        pl.semaphore_signal(barrier, inc=1, device_id={"tp": z + 1}, device_id_type=MESH)
    at_end = (z == 0) | (z == n_z - 1)

    @pl.when(at_end)
    def _():
        pl.semaphore_wait(barrier, 3)

    @pl.when(jnp.logical_not(at_end))
    def _():
        pl.semaphore_wait(barrier, 4)

    def at(j):
        return pl.ds(j * size, size)

    def d_copy(j, side):
        owner = far_pair if side == 0 else pair
        return pltpu.make_async_remote_copy(
            part.at[pl.ds(owner * rows + j * size, size)], near.at[side, at(j)],
            d_send.at[side, j], d_recv.at[side, j], device_id={"ep": pair}, device_id_type=MESH)

    def m_copy(j, side):
        owner = far if side == 0 else e
        return pltpu.make_async_copy(part.at[pl.ds(owner * rows + j * size, size)], mine.at[side, at(j)], m_sem.at[side, j])

    def y_copy(j):
        return pltpu.make_async_remote_copy(
            mine.at[0, at(j)], far_in.at[at(j)], y_send.at[j], y_recv.at[j], device_id={"ep": far}, device_id_type=MESH)

    def z_copy(j, slot, to):
        return pltpu.make_async_remote_copy(
            mine.at[1, at(j)], zin.at[slot, at(j)], z_send.at[j], z_recv.at[slot, j], device_id={"tp": to}, device_id_type=MESH)

    def t_copy(j, side, to, src):
        return pltpu.make_async_remote_copy(
            src, zin.at[1, at(j)], t_send.at[side, j], z_recv.at[1, j], device_id={"tp": to}, device_id_type=MESH)

    def first(j, _):
        for side in range(2):
            d_copy(j, side).start()
            m_copy(j, side).start()
        return 0
    lax.fori_loop(0, n_chunk, first, 0)

    def f32(ref):
        return ref[...].astype(jnp.float32)

    def finish(j, src):
        def put(g, _):
            for u in range(8):
                i = g * 8 + u
                t4[pl.ds(i, chunks, stride=size + 1), :] = src[i].astype(jnp.float32)
            return 0
        lax.fori_loop(0, size // 8, put, 0)
        for k in range(chunks):
            cols = slice(k * LANES, (k + 1) * LANES)
            tot = t4[k * (size + 1):k * (size + 1) + size, :]
            out_ref[at(j), cols] = (hid[at(j), cols].astype(jnp.float32) + tot).astype(jnp.bfloat16)

    def step(i, _):
        @pl.when(i < n_chunk)
        def _():
            for side in range(2):
                d_copy(i, side).wait_recv()
                m_copy(i, side).wait()
            mine[0, at(i)] = (f32(mine.at[0, at(i)]) + f32(near.at[0, at(i)])).astype(jnp.bfloat16)
            y_copy(i).start()

        def stage(shift):
            j = i - shift * lag
            odd = j % 2
            spot = z + odd * (n_z - 1 - 2 * z)
            ahead = 1 - 2 * odd
            return j, spot, ahead, (j >= 0) & (j < n_chunk)

        j, spot, ahead, live = stage(1)

        @pl.when(live)
        def _():
            y_copy(j).wait_recv()
            mine[1, at(j)] = (f32(mine.at[1, at(j)]) + f32(near.at[1, at(j)]) + f32(far_in.at[at(j)])).astype(jnp.bfloat16)

            @pl.when(spot == 0)
            def _():
                z_copy(j, 0, z + ahead).start()

            @pl.when(spot == 3)
            def _():
                z_copy(j, 0, z - ahead).start()

        j2, spot2, ahead2, live2 = stage(2)

        @pl.when(live2 & (spot2 == 2))
        def _():
            z_copy(j2, 0, zn).wait_recv()
            mine[1, at(j2)] = (f32(mine.at[1, at(j2)]) + f32(zin.at[0, at(j2)])).astype(jnp.bfloat16)
            z_copy(j2, 1, z - ahead2).start()

        j3, spot3, ahead3, live3 = stage(3)

        @pl.when(live3 & (spot3 == 1))
        def _():
            z_copy(j3, 0, zn).wait_recv()
            z_copy(j3, 1, zn).wait_recv()
            mine[1, at(j3)] = (f32(mine.at[1, at(j3)]) + f32(zin.at[0, at(j3)]) + f32(zin.at[1, at(j3)])).astype(jnp.bfloat16)
            t_copy(j3, 0, z - ahead3, mine.at[1, at(j3)]).start()
            t_copy(j3, 1, z + ahead3, mine.at[1, at(j3)]).start()
            finish(j3, mine.at[1, at(j3)])

        j4, spot4, ahead4, live4 = stage(4)

        @pl.when(live4 & (spot4 == 2))
        def _():
            z_copy(j4, 1, zn).wait_recv()
            t_copy(j4, 0, z + ahead4, zin.at[1, at(j4)]).start()
            finish(j4, zin.at[1, at(j4)])

        j5, spot5, ahead5, live5 = stage(5)

        @pl.when(live5 & ((spot5 == 0) | (spot5 == 3)))
        def _():
            z_copy(j5, 1, zn).wait_recv()
            finish(j5, zin.at[1, at(j5)])
        return 0
    lax.fori_loop(0, n_chunk + 5 * lag, step, 0)

    def drain(j, _):
        odd = j % 2
        spot = z + odd * (n_z - 1 - 2 * z)
        d_copy(j, 0).wait_send()
        d_copy(j, 1).wait_send()
        y_copy(j).wait_send()

        @pl.when(spot != 1)
        def _():
            z_copy(j, 0, zn).wait_send()

        @pl.when((spot == 1) | (spot == 2))
        def _():
            t_copy(j, 0, zn, mine.at[1, at(j)]).wait_send()

        @pl.when(spot == 1)
        def _():
            t_copy(j, 1, zn, mine.at[1, at(j)]).wait_send()
        return 0
    lax.fori_loop(0, n_chunk, drain, 0)


def combine(part, hidden_in, n_chunk, lag):
    rows, hidden = hidden_in.shape
    block = (rows,) + part.shape[1:]
    dma = pltpu.SemaphoreType.DMA
    size = rows // n_chunk
    hbm = pl.BlockSpec(memory_space=pl.ANY)
    return pl.pallas_call(
        functools.partial(combine_kernel, n_chunk, lag),
        out_shape=jax.ShapeDtypeStruct((rows, hidden), jnp.bfloat16),
        in_specs=[hbm, pl.BlockSpec(memory_space=pltpu.VMEM)],
        out_specs=pl.BlockSpec(memory_space=pltpu.VMEM),
        scratch_shapes=[
            pltpu.VMEM((2,) + block, jnp.bfloat16), pltpu.VMEM((2,) + block, jnp.bfloat16), pltpu.VMEM(block, jnp.bfloat16),
            pltpu.VMEM((2,) + block, jnp.bfloat16),
            pltpu.VMEM(((size + 1) * part.shape[1] + 8, LANES), jnp.float32),
            dma((2, n_chunk)), dma((2, n_chunk)), dma((2, n_chunk)), dma((n_chunk,)), dma((n_chunk,)),
            dma((n_chunk,)), dma((2, n_chunk)), dma((2, n_chunk)),
        ],
        compiler_params=pltpu.CompilerParams(collective_id=1, has_side_effects=True, vmem_limit_bytes=40 << 20),
        name="combine",
    )(part, hidden_in)


def solution(mesh):
    tok_spec = P(('dp', 'ep'), None)
    in_specs = (tok_spec, tok_spec, P(None), P(None, None), P(None, None),
                P('ep', None, 'tp'), P('ep', None, 'tp'), P('ep', 'tp', None),
                P(None, ('tp', 'ep')), P(None, ('tp', 'ep')), P(('tp', 'ep'), None))

    def local_step(hidden_in, topk_idx, norm_gain, router_w, shared_sig_w, exp_gate, exp_up, exp_down, sh_gate, sh_up, sh_down):
        all_h, sums, wt, all_idx = front(hidden_in, norm_gain, router_w.T, shared_sig_w.T, topk_idx.T,
                                         lax.axis_size('ep'), sh_gate.T, sh_up.T, sh_down)
        part = moe(all_idx, wt.reshape(-1), all_h, sums, jnp.swapaxes(exp_gate, 1, 2), jnp.swapaxes(exp_up, 1, 2), exp_down)
        return combine(part, hidden_in, COMBINE_CHUNKS, COMBINE_LAG)

    return jax.shard_map(local_step, mesh=mesh, in_specs=in_specs, out_specs=tok_spec, check_vma=False)
```
